128 devices in a mesh: gx: 2 (over core), gy: 64 (over z, y, x).
Axes of the slice: x: 4, y: 4, z: 4, core: 2. Of those that a mesh axis runs over, the one named last changes fastest.
Arguments:
- right_side: float32 [128, 16384], P('gx', 'gy'), may hold values from -34 to 34, as said below
- initial: float32 [128, 16384], P('gx', 'gy'), may hold values from -0.6 to 0.6
- reaction: float32 [128, 16384], P('gx', 'gy'), may hold values from 0.05 to 0.5
- velocity_x: float32 [128, 16384], P('gx', 'gy'), may hold values from -1 to 1
- velocity_y: float32 [128, 16384], P('gx', 'gy'), may hold values from -1 to 1
Outputs:
- solution: float32 [128, 16384], P('gx', 'gy')
- residual: float32 [128, 16384], P('gx', 'gy')
The draws below stay inside these ranges and needn't reach their ends.
Inputs may be any that keep to these rules, and one draw needn't show every extreme that they name: right_side is noise bounded by 4 in size times an envelope 0.5 + 8 g, where g is a periodic Gaussian bump of one device block's width along each dimension centred at a drawn position, so its entries lie within -34 and 34.
All inputs are finite; a program needn't handle non-finite values.
Results may differ from the reference program's by a relative error of at most 0.0075.
Values sent between devices are 32-bit elements.
A program may use at most 64 MiB of HBM per device.

```python
import math
import jax
import jax.numpy as jnp
from jax import lax

CX = 64
CY = 256
RESTART = 15
NX = 128
NY = 16384


def draw_right_side(key, part):
    noise_key = jax.random.fold_in(key, 11)
    centre_key = jax.random.fold_in(key, 12)
    noise = jnp.clip(jax.random.normal(noise_key, (NX, NY), jnp.float32), -4.0, 4.0)
    centre = jax.random.uniform(centre_key, (2,), jnp.float32)
    along_x = jnp.mod(jnp.arange(NX, dtype=jnp.float32) - centre[0] * NX, NX)
    along_y = jnp.mod(jnp.arange(NY, dtype=jnp.float32) - centre[1] * NY, NY)
    gap_x = jnp.minimum(along_x, NX - along_x) / CX
    gap_y = jnp.minimum(along_y, NY - along_y) / CY
    bump = jnp.exp(-0.5 * (gap_x[:, None] * gap_x[:, None] + gap_y[None, :] * gap_y[None, :]))
    return noise * (0.5 + 8.0 * bump)


def block_levels(key, dims, pieces, smallest, top_value):
    def one(dim, parts):
        draws = jax.random.uniform(jax.random.fold_in(jax.random.fold_in(key, 6), dim), (parts,), jnp.float32, smallest / len(pieces), top_value / len(pieces))
        return jnp.repeat(jnp.exp(draws), dims[dim] // parts).reshape((-1,) + (1,) * (len(dims) - dim - 1))

    gain = one(*pieces[0])
    for cut in pieces[1:]:
        gain = gain * one(*cut)
    return gain


def scatter_about(stream_key, extent, deviation, limit, split=(), held_as=jnp.bfloat16):
    loudness = block_levels(stream_key, extent, split, -0.22, 0.18) if split else 1.0
    drawn = jax.random.normal(stream_key, extent, jnp.float32) * deviation * loudness
    return jnp.minimum(jnp.maximum(drawn, -limit), limit).astype(held_as)


def setup_inputs(seed: int = 0) -> dict:
    arg_keys = jax.random.split(jax.random.key(seed), 6)
    return {
        "right_side": draw_right_side(jax.random.fold_in(arg_keys[5], 71), 0),
        "initial": scatter_about(arg_keys[1], (NX, NY), 0.1, 0.6, ((0, 2), (1, 64)), jnp.float32),
        "reaction": jnp.clip(jnp.exp(math.log(0.5) - 2.3025851 * jax.random.uniform(arg_keys[2], (NX, NY), jnp.float32) ** block_levels(arg_keys[2], (NX, NY), ((0, 2), (1, 64)), -0.2, 0.2)), 0.05, 0.5),
        "velocity_x": jnp.clip(jax.random.uniform(arg_keys[3], (NX, NY), jnp.float32, -1.0, 1.0) * block_levels(arg_keys[3], (NX, NY), ((0, 2), (1, 64)), -0.4, 0.0), -1.0, 1.0),
        "velocity_y": jnp.clip(jax.random.uniform(arg_keys[4], (NX, NY), jnp.float32, -1.0, 1.0) * block_levels(arg_keys[4], (NX, NY), ((0, 2), (1, 64)), -0.4, 0.0), -1.0, 1.0),
    }


def moved(field, offset, dimension):
    return jnp.roll(field, -offset, dimension)

def first_diff(field, dimension):
    outer = moved(field, -2, dimension) - moved(field, 2, dimension)
    inner = moved(field, 1, dimension) - moved(field, -1, dimension)
    return (outer + 8.0 * inner) / 12.0

def second_diff(field, dimension):
    inner = moved(field, 1, dimension) + moved(field, -1, dimension)
    outer = moved(field, 2, dimension) + moved(field, -2, dimension)
    return (16.0 * inner - outer - 30.0 * field) / 12.0

def operate(field, reaction, velocity_x, velocity_y):
    diffusion = second_diff(field, 0) + second_diff(field, 1)
    advect_x = 0.5 * (velocity_x * first_diff(field, 0) + first_diff(velocity_x * field, 0))
    advect_y = 0.5 * (velocity_y * first_diff(field, 1) + first_diff(velocity_y * field, 1))
    return reaction * field - diffusion + advect_x + advect_y

def least_squares(hessenberg, beta):
    columns_total = hessenberg.shape[1]
    target = jnp.where(jnp.arange(columns_total + 1) == 0, beta, 0.0)

    def rotate(column, carried):
        upper, target = carried
        top_row = upper[column]
        next_row = upper[column + 1]
        diagonal_entry = top_row[column]
        below_entry = next_row[column]
        radius = jnp.sqrt(diagonal_entry * diagonal_entry + below_entry * below_entry)
        cosine = diagonal_entry / radius
        sine_value = below_entry / radius
        upper = upper.at[column].set(cosine * top_row + sine_value * next_row)
        upper = upper.at[column + 1].set(cosine * next_row - sine_value * top_row)
        upper_value = target[column]
        lower_value = target[column + 1]
        target = target.at[column].set(cosine * upper_value + sine_value * lower_value)
        target = target.at[column + 1].set(cosine * lower_value - sine_value * upper_value)
        return (upper, target)
    upper, target = lax.fori_loop(0, columns_total, rotate, (hessenberg, target))

    def substitute(count, weights):
        row_index = columns_total - 1 - count
        known = jnp.sum(upper[row_index] * weights)
        return weights.at[row_index].set((target[row_index] - known) / upper[row_index, row_index])
    return lax.fori_loop(0, columns_total, substitute, jnp.zeros((columns_total,), jnp.float32))

def reference(right_side, initial, reaction, velocity_x, velocity_y):

    def operator_on(field):
        return operate(field, reaction, velocity_x, velocity_y)
    start_residual = right_side - operator_on(initial)
    beta = jnp.sqrt(jnp.sum(start_residual * start_residual))
    basis = [start_residual / beta]
    hessenberg = jnp.zeros((RESTART + 1, RESTART), jnp.float32)
    for column in range(RESTART):
        applied = operator_on(basis[column])
        projection = jnp.stack([jnp.sum(vector * applied) for vector in basis])
        correction = jnp.zeros_like(applied)
        for position, vector in enumerate(basis):
            correction = correction + projection[position] * vector
        applied = applied - correction
        length = jnp.sqrt(jnp.sum(applied * applied))
        hessenberg = hessenberg.at[:column + 1, column].set(projection)
        hessenberg = hessenberg.at[column + 1, column].set(length)
        basis.append(applied / length)
    weights = least_squares(hessenberg, beta)
    solution = initial
    for position in range(RESTART):
        solution = solution + weights[position] * basis[position]
    residual = right_side - operator_on(solution)
    return (solution, residual)
```

```python
import functools
import itertools

import jax
import jax.numpy as jnp
from jax import lax
from jax.experimental import pallas as pl
from jax.experimental.pallas import tpu as pltpu
from jax.sharding import Mesh
from jax.sharding import PartitionSpec as P

RESTART = 15
VECTORS = RESTART + 1
GY = ("gy_0", "gy_1", "gy_2")
AXES = ("gx",) + GY
PHASES = (("gx", "gy_2"), ("gy_1",), ("gy_0",))
DEPTH = 32
GROUPS = 4
STEPS = 16
SHIFT, SCALE, BACK = 5.525, 2.72, 0.94
B, X0, RE, VX, VY = 0, 1, 2, 3, 4
PACKED = (X0, RE, VX, VY)


def values_at_zero():
    values = [1.0, -SHIFT / SCALE]
    for _ in range(VECTORS - 2):
        values.append(-(SHIFT / SCALE) * values[-1] - BACK * values[-2])
    return values


def kernel(sizes, *refs):
    inputs = refs[:5]
    outputs = refs[5:7]
    (block, pack, halo, coef, field, basis, mirror, gram_parts, out) = refs[7:16]
    phases = [p for p in PHASES if any(sizes[a] > 1 for a in p)]
    reduce_bufs = refs[16 : 16 + len(phases)]
    (load_sem, swap_sem, halo_send, halo_recv, mirror_sem, out_sem) = refs[
        16 + len(phases) : 22 + len(phases)
    ]
    reduce_sems = refs[22 + len(phases) :]

    place = {a: lax.axis_index(a) for a in AXES}
    core = place["gx"]
    sibling = {"gx": 1 - core}

    def along(step):
        total = sizes["gy_0"] * sizes["gy_1"] * sizes["gy_2"]
        flat = (place["gy_0"] * sizes["gy_1"] + place["gy_1"]) * sizes["gy_2"] + place["gy_2"]
        flat = lax.rem(flat + step + total, total)
        low = lax.rem(flat, sizes["gy_2"])
        rest = lax.div(flat, sizes["gy_2"])
        return lax.div(rest, sizes["gy_1"]), lax.rem(rest, sizes["gy_1"]), low

    right, left = along(1), along(-1)

    def at(chip, core_index):
        return {"gx": core_index, "gy_0": chip[0], "gy_1": chip[1], "gy_2": chip[2]}

    def group_of(axes):
        offsets = list(itertools.product(*[range(sizes[a]) for a in axes]))
        peers = []
        for offset in offsets:
            where = {a: lax.rem(place[a] + o, sizes[a]) for a, o in zip(axes, offset)}
            slot = 0
            for a in axes:
                slot = slot * sizes[a] + where[a]
            peers.append((where, slot))
        return peers

    groups = [group_of(axes) for axes in phases]

    loads = []
    for a in range(5):
        for tile in range(2):
            loads.append(
                pltpu.make_async_copy(
                    inputs[a].at[:, pl.ds(128 * tile, 128)],
                    block.at[a, tile, pl.ds(0, 64), :],
                    load_sem.at[a, tile],
                )
            )
            loads[-1].start()
    barrier = pltpu.get_barrier_semaphore()
    greeted = 0
    to_greet = [at(right, 0), at(right, 1), at(left, 0), at(left, 1), sibling]
    for group in groups:
        to_greet += [where for where, _ in group[1:]]
    for device in to_greet:
        pl.semaphore_signal(barrier, inc=1, device_id=device, device_id_type=pl.DeviceIdType.MESH)
        greeted += 1
    for load in loads:
        load.wait()

    lane = lax.broadcasted_iota(jnp.int32, (8, 128), 1)
    row = lax.broadcasted_iota(jnp.int32, (8, 128), 0)

    for i in range(8):
        rows = pl.ds(8 * i, 8)
        for side, tile, first in ((0, 1, 96), (1, 0, 0)):
            value = block[PACKED[0], tile, rows, :]
            for g in range(1, GROUPS):
                start = (first + DEPTH * g) % 128
                moved = pltpu.roll(block[PACKED[g], tile, rows, :], DEPTH * g, 1)
                inside = (lane >= start) & (lane < start + DEPTH)
                value = jnp.where(inside, moved, value)
            pack[side, rows, :] = value

    pl.semaphore_wait(barrier, greeted)

    swap = pltpu.make_async_remote_copy(
        block.at[:, :, pl.ds(0, 64), :],
        block.at[:, :, pl.ds(64, 64), :],
        swap_sem.at[0],
        swap_sem.at[1],
        device_id=sibling,
        device_id_type=pl.DeviceIdType.MESH,
    )
    swap.start()
    sends = []
    for side, chip, target in ((0, right, 0), (1, left, 1)):
        same = core if target == 0 else 1 - core
        for part in range(2):
            source = pack.at[side] if part == 0 else block.at[B, 1 - side, pl.ds(0, 64), :]
            copy = pltpu.make_async_remote_copy(
                source,
                halo.at[part, pl.ds(pl.multiple_of(64 * same, 64), 64), :],
                halo_send.at[side, part],
                halo_recv.at[part, same],
                device_id=at(chip, target),
                device_id_type=pl.DeviceIdType.MESH,
            )
            copy.start()
            sends.append(copy)
    swap.wait()
    for part in range(2):
        for half in range(2):
            pltpu.make_async_remote_copy(
                halo.at[part, pl.ds(64 * half, 64), :],
                halo.at[part, pl.ds(64 * half, 64), :],
                halo_send.at[0, part],
                halo_recv.at[part, half],
                device_id=sibling,
                device_id_type=pl.DeviceIdType.MESH,
            ).wait_recv()

    far = 1 - core
    first = jnp.where(core == 0, 96, 0)
    from_chip = (lane >= first) & (lane < first + DEPTH)
    for a in range(5):
        for t in range(STEPS):
            strided = pl.ds(t, 8, stride=STEPS)
            field[a, t, :, 0:128] = block[a, core, strided, :]
            if a == B:
                edge = halo[1, strided, :]
            else:
                g = PACKED.index(a)
                edge = halo[0, strided, :]
                if g:
                    edge = pltpu.roll(edge, 128 - DEPTH * g, 1)
            field[a, t, :, 128:256] = jnp.where(from_chip, edge, block[a, far, strided, :])

    def row_shift(load, t):
        if t >= STEPS:
            return pltpu.roll(load(t - STEPS), 7, 0)
        if t < 0:
            return pltpu.roll(load(t + STEPS), 1, 0)
        return load(t)

    def column_shift(value, offset):
        return pltpu.roll(value, (-offset) % 256, 1)

    inv = 1.0 / SCALE
    for t in range(STEPS):
        speed = lambda i: field[VX, i]
        here = speed(t)
        coef[0, t] = (field[RE, t] + (5.0 - SHIFT)) * inv
        coef[1, t] = (here + row_shift(speed, t + 1)) * (inv / 3.0) - 4.0 / 3.0 * inv
        coef[2, t] = (here + row_shift(speed, t - 1)) * (-inv / 3.0) - 4.0 / 3.0 * inv
        coef[3, t] = (here + row_shift(speed, t + 2)) * (-inv / 24.0) + inv / 12.0
        coef[4, t] = (here + row_shift(speed, t - 2)) * (inv / 24.0) + inv / 12.0
        here = field[VY, t]
        coef[5, t] = (here + column_shift(here, 1)) * (inv / 3.0) - 4.0 / 3.0 * inv
        coef[6, t] = (here + column_shift(here, -1)) * (-inv / 3.0) - 4.0 / 3.0 * inv
        coef[7, t] = (here + column_shift(here, 2)) * (-inv / 24.0) + inv / 12.0
        coef[8, t] = (here + column_shift(here, -2)) * (inv / 24.0) + inv / 12.0

    def operate(load, t):
        here = load(t)
        value = coef[0, t] * here
        value += coef[1, t] * row_shift(load, t + 1)
        value += coef[2, t] * row_shift(load, t - 1)
        value += coef[3, t] * row_shift(load, t + 2)
        value += coef[4, t] * row_shift(load, t - 2)
        value += coef[5, t] * column_shift(here, 1)
        value += coef[6, t] * column_shift(here, -1)
        value += coef[7, t] * column_shift(here, 2)
        value += coef[8, t] * column_shift(here, -2)
        return value

    for t in range(STEPS):
        load = lambda i: field[X0, i]
        basis[0, t] = jnp.zeros((8, 256), jnp.float32)
        basis[1, t] = field[B, t] - SCALE * operate(load, t) - SHIFT * load(t)

    def grow(k, carry):
        for t in range(STEPS):
            load = lambda i: basis[k + 1, i]
            basis[k + 2, t] = operate(load, t) - BACK * basis[k, t]
        return carry

    lax.fori_loop(0, RESTART, grow, 0)

    size = 4
    for bi in range(VECTORS // size):
        for bj in range(bi + 1):
            pairs = [
                (i, j)
                for i in range(bi * size, bi * size + size)
                for j in range(bj * size, bj * size + size)
                if j <= i
            ]
            sums = {}
            for t in range(STEPS):
                need = sorted({i for pair in pairs for i in pair})
                cells = {i: basis[i + 1, t, :, 0:128] for i in need}
                for i, j in pairs:
                    product = cells[i] * cells[j]
                    sums[i, j] = product if t == 0 else sums[i, j] + product
            for i, j in pairs:
                total = jnp.sum(sums[i, j], axis=0, keepdims=True)
                gram_parts[i, j : j + 1, :] = total
                if i != j:
                    gram_parts[j, i : i + 1, :] = total

    packed = jnp.zeros((8, 128), jnp.float32)
    for k in range(VECTORS):
        for half in range(2):
            total = jnp.sum(gram_parts[k, 8 * half : 8 * half + 8, :], axis=1, keepdims=True)
            packed = jnp.where(lane == 2 * k + half, total, packed)

    mirror_copy = pltpu.make_async_remote_copy(
        basis.at[pl.ds(1, VECTORS), :, :, pl.ds(0, 128)],
        mirror,
        mirror_sem.at[0],
        mirror_sem.at[1],
        device_id=sibling,
        device_id_type=pl.DeviceIdType.MESH,
    )
    for p, group in enumerate(groups):
        buf = reduce_bufs[p]
        send_sem, recv_sem = reduce_sems[2 * p], reduce_sems[2 * p + 1]
        mine = group[0][1]
        buf[mine] = packed
        copies = []
        for n, (where, slot) in enumerate(group[1:]):
            copy = pltpu.make_async_remote_copy(
                buf.at[mine],
                buf.at[mine],
                send_sem.at[n],
                recv_sem.at[mine],
                device_id=where,
                device_id_type=pl.DeviceIdType.MESH,
            )
            copy.start()
            copies.append(copy)
        if p == 0:
            mirror_copy.start()
        for n, (where, slot) in enumerate(group[1:]):
            pltpu.make_async_remote_copy(
                buf.at[slot],
                buf.at[slot],
                send_sem.at[n],
                recv_sem.at[slot],
                device_id=where,
                device_id_type=pl.DeviceIdType.MESH,
            ).wait_recv()
        packed = buf[0]
        for slot in range(1, len(group)):
            packed = packed + buf[slot]
        sends += copies
    mirror_copy.wait()

    values = values_at_zero()
    columns = []
    for k in range(VECTORS):
        columns.append(
            [
                jnp.broadcast_to(packed[:, 2 * k + h : 2 * k + h + 1], (8, 128))
                for h in range(2)
            ]
        )
    start = []
    for h in range(2):
        value = jnp.full((8, 128), values[8 * h], jnp.float32)
        for s in range(1, 8):
            value = jnp.where(row == s, values[8 * h + s], value)
        start.append(value)
    columns.append(list(start))

    def entry(column, i):
        return jnp.broadcast_to(column[i // 8][i % 8 : i % 8 + 1, :], (8, 128))

    for k in range(VECTORS):
        pivot = columns[k]
        inverse = 1.0 / entry(pivot, k)
        for j in range(k + 1, VECTORS + 1):
            factor = (entry(pivot, j) if j < VECTORS else entry(columns[j], k)) * inverse
            for h in range(2):
                columns[j][h] = columns[j][h] - pivot[h] * factor
            columns[j][k // 8] = jnp.where(row == k % 8, factor, columns[j][k // 8])
    u = columns[VECTORS]
    norm = jnp.sum(start[0] * u[0] + start[1] * u[1], axis=0, keepdims=True)
    inverse = jnp.broadcast_to(1.0 / norm, (8, 128))
    left_over = [entry(u, j) * inverse for j in range(VECTORS)]
    weights = [None] * RESTART
    for j in range(RESTART, 0, -1):
        value = left_over[j] * (-1.0 / SCALE)
        if j + 1 < RESTART:
            value = value - BACK * weights[j + 1]
        if j < RESTART:
            value = value - (SHIFT / SCALE) * weights[j]
        weights[j - 1] = value

    for t in range(STEPS):
        strided = pl.ds(t, 8, stride=STEPS)
        near = row < 4
        answer = jnp.where(
            near, block[X0, core, strided, :], pltpu.roll(block[X0, far, strided, :], 4, 0)
        )
        residual = jnp.zeros((8, 128), jnp.float32)
        for k in range(VECTORS):
            cells = jnp.where(near, basis[k + 1, t, :, 0:128], mirror[k, t])
            residual = residual + left_over[k] * cells
            if k < RESTART:
                answer = answer + weights[k] * cells
        out[0, strided, :] = answer
        out[1, strided, :] = residual

    stores = []
    for o in range(2):
        for part in range(2):
            tile = core if part == 0 else far
            copy = pltpu.make_async_copy(
                out.at[o, pl.ds(64 * part, 64), :],
                outputs[o].at[:, pl.ds(pl.multiple_of(128 * tile, 128), 128)],
                out_sem.at[o, part],
            )
            copy.start()
            stores.append(copy)
    for copy in sends:
        copy.wait_send()
    for copy in stores:
        copy.wait()


def per_device(sizes, *arrays):
    phases = [p for p in PHASES if any(sizes[a] > 1 for a in p)]
    counts = []
    for axes in phases:
        count = 1
        for a in axes:
            count *= sizes[a]
        counts.append(count)
    f32 = jnp.float32
    dma = pltpu.SemaphoreType.DMA
    reduce_sems = []
    for count in counts:
        reduce_sems += [dma((count,)), dma((count,))]
    shape = jax.ShapeDtypeStruct((64, 256), f32)
    return pl.pallas_call(
        functools.partial(kernel, sizes),
        out_shape=(shape, shape),
        in_specs=[pl.BlockSpec(memory_space=pl.ANY)] * 5,
        out_specs=(pl.BlockSpec(memory_space=pl.ANY),) * 2,
        scratch_shapes=[
            pltpu.VMEM((5, 2, 128, 128), f32),
            pltpu.VMEM((2, 64, 128), f32),
            pltpu.VMEM((2, 128, 128), f32),
            pltpu.VMEM((9, STEPS, 8, 256), f32),
            pltpu.VMEM((5, STEPS, 8, 256), f32),
            pltpu.VMEM((VECTORS + 1, STEPS, 8, 256), f32),
            pltpu.VMEM((VECTORS, STEPS, 8, 128), f32),
            pltpu.VMEM((VECTORS, VECTORS, 128), f32),
            pltpu.VMEM((2, 128, 128), f32),
        ]
        + [pltpu.VMEM((count, 8, 128), f32) for count in counts]
        + [
            dma((5, 2)),
            dma((2,)),
            dma((2, 2)),
            dma((2, 2)),
            dma((2,)),
            dma((2, 2)),
        ]
        + reduce_sems,
        compiler_params=pltpu.CompilerParams(collective_id=0, has_side_effects=True),
    )(*arrays)


def solution(mesh):
    counts = (4, 4, 4) if mesh.shape["gy"] == 64 else (1, 2, mesh.shape["gy"] // 2)
    torus = Mesh(mesh.devices.reshape((mesh.shape["gx"],) + counts), AXES)
    spec = P("gx", GY)
    return jax.shard_map(
        functools.partial(per_device, dict(torus.shape)),
        mesh=torus,
        in_specs=(spec,) * 5,
        out_specs=(spec, spec),
        check_vma=False,
    )
```

```python
import functools

import jax
import jax.numpy as jnp
from jax import lax
from jax.experimental import pallas as pl
from jax.experimental.pallas import tpu as pltpu
from jax.sharding import Mesh
from jax.sharding import PartitionSpec as P

RESTART = 15
VECTORS = RESTART + 1
GY = ("gy_0", "gy_1", "gy_2")
AXES = ("gx",) + GY
LOGICAL = pl.DeviceIdType.LOGICAL
DEPTH = 32
GROUPS = 4
STEPS = 16
SHIFT, SCALE, BACK = 5.525, 2.72, 0.94
B, X0, RE, VX, VY = 0, 1, 2, 3, 4
PACKED = (X0, RE, VX, VY)


def values_at_zero():
    values = [1.0, -SHIFT / SCALE]
    for _ in range(VECTORS - 2):
        values.append(-(SHIFT / SCALE) * values[-1] - BACK * values[-2])
    return values


def kernel(sizes, *refs):
    inputs = refs[:5]
    outputs = refs[5:7]
    (block, pack, halo, coef, field, basis, mirror, gram_parts, out) = refs[7:16]
    (gathered, share) = refs[16:18]
    (load_sem, swap_sem, halo_send, halo_recv, mirror_sem, out_sem, send_sem, recv_sem) = refs[18:]
    devices = 1
    for a in AXES:
        devices *= sizes[a]

    place = {a: lax.axis_index(a) for a in AXES}
    core = place["gx"]
    sibling = {"gx": 1 - core}

    def along(step):
        total = sizes["gy_0"] * sizes["gy_1"] * sizes["gy_2"]
        flat = (place["gy_0"] * sizes["gy_1"] + place["gy_1"]) * sizes["gy_2"] + place["gy_2"]
        flat = lax.rem(flat + step + total, total)
        low = lax.rem(flat, sizes["gy_2"])
        rest = lax.div(flat, sizes["gy_2"])
        return lax.div(rest, sizes["gy_1"]), lax.rem(rest, sizes["gy_1"]), low

    right, left = along(1), along(-1)

    def at(chip, core_index):
        return {"gx": core_index, "gy_0": chip[0], "gy_1": chip[1], "gy_2": chip[2]}

    me = core
    for a in GY:
        me = me * sizes[a] + place[a]

    loads = []
    for a in range(5):
        for tile in range(2):
            loads.append(
                pltpu.make_async_copy(
                    inputs[a].at[:, pl.ds(128 * tile, 128)],
                    block.at[a, tile, pl.ds(0, 64), :],
                    load_sem.at[a, tile],
                )
            )
            loads[-1].start()
    barrier = pltpu.get_barrier_semaphore()
    for o in range(1, devices):
        pl.semaphore_signal(
            barrier, inc=1, device_id=lax.rem(me + o, devices), device_id_type=LOGICAL
        )
    for load in loads:
        load.wait()

    lane = lax.broadcasted_iota(jnp.int32, (8, 128), 1)
    row = lax.broadcasted_iota(jnp.int32, (8, 128), 0)

    for i in range(8):
        rows = pl.ds(8 * i, 8)
        for side, tile, first in ((0, 1, 96), (1, 0, 0)):
            value = block[PACKED[0], tile, rows, :]
            for g in range(1, GROUPS):
                start = (first + DEPTH * g) % 128
                moved = pltpu.roll(block[PACKED[g], tile, rows, :], DEPTH * g, 1)
                inside = (lane >= start) & (lane < start + DEPTH)
                value = jnp.where(inside, moved, value)
            pack[side, rows, :] = value

    pl.semaphore_wait(barrier, devices - 1)

    swap = pltpu.make_async_remote_copy(
        block.at[:, :, pl.ds(0, 64), :],
        block.at[:, :, pl.ds(64, 64), :],
        swap_sem.at[0],
        swap_sem.at[1],
        device_id=sibling,
        device_id_type=pl.DeviceIdType.MESH,
    )
    swap.start()
    sends = []
    for side, chip, target in ((0, right, 0), (1, left, 1)):
        same = core if target == 0 else 1 - core
        for part in range(2):
            source = pack.at[side] if part == 0 else block.at[B, 1 - side, pl.ds(0, 64), :]
            copy = pltpu.make_async_remote_copy(
                source,
                halo.at[part, pl.ds(pl.multiple_of(64 * same, 64), 64), :],
                halo_send.at[side, part],
                halo_recv.at[part, same],
                device_id=at(chip, target),
                device_id_type=pl.DeviceIdType.MESH,
            )
            copy.start()
            sends.append(copy)
    swap.wait()
    for part in range(2):
        for half in range(2):
            pltpu.make_async_remote_copy(
                halo.at[part, pl.ds(64 * half, 64), :],
                halo.at[part, pl.ds(64 * half, 64), :],
                halo_send.at[0, part],
                halo_recv.at[part, half],
                device_id=sibling,
                device_id_type=pl.DeviceIdType.MESH,
            ).wait_recv()

    far = 1 - core
    first = jnp.where(core == 0, 96, 0)
    from_chip = (lane >= first) & (lane < first + DEPTH)
    for a in range(5):
        for t in range(STEPS):
            strided = pl.ds(t, 8, stride=STEPS)
            field[a, t, :, 0:128] = block[a, core, strided, :]
            if a == B:
                edge = halo[1, strided, :]
            else:
                g = PACKED.index(a)
                edge = halo[0, strided, :]
                if g:
                    edge = pltpu.roll(edge, 128 - DEPTH * g, 1)
            field[a, t, :, 128:256] = jnp.where(from_chip, edge, block[a, far, strided, :])

    def row_shift(load, t):
        if t >= STEPS:
            return pltpu.roll(load(t - STEPS), 7, 0)
        if t < 0:
            return pltpu.roll(load(t + STEPS), 1, 0)
        return load(t)

    def column_shift(value, offset):
        return pltpu.roll(value, (-offset) % 256, 1)

    inv = 1.0 / SCALE
    for t in range(STEPS):
        speed = lambda i: field[VX, i]
        here = speed(t)
        coef[0, t] = (field[RE, t] + (5.0 - SHIFT)) * inv
        coef[1, t] = (here + row_shift(speed, t + 1)) * (inv / 3.0) - 4.0 / 3.0 * inv
        coef[2, t] = (here + row_shift(speed, t - 1)) * (-inv / 3.0) - 4.0 / 3.0 * inv
        coef[3, t] = (here + row_shift(speed, t + 2)) * (-inv / 24.0) + inv / 12.0
        coef[4, t] = (here + row_shift(speed, t - 2)) * (inv / 24.0) + inv / 12.0
        here = field[VY, t]
        coef[5, t] = (here + column_shift(here, 1)) * (inv / 3.0) - 4.0 / 3.0 * inv
        coef[6, t] = (here + column_shift(here, -1)) * (-inv / 3.0) - 4.0 / 3.0 * inv
        coef[7, t] = (here + column_shift(here, 2)) * (-inv / 24.0) + inv / 12.0
        coef[8, t] = (here + column_shift(here, -2)) * (inv / 24.0) + inv / 12.0

    def operate(load, t):
        here = load(t)
        value = coef[0, t] * here
        value += coef[1, t] * row_shift(load, t + 1)
        value += coef[2, t] * row_shift(load, t - 1)
        value += coef[3, t] * row_shift(load, t + 2)
        value += coef[4, t] * row_shift(load, t - 2)
        value += coef[5, t] * column_shift(here, 1)
        value += coef[6, t] * column_shift(here, -1)
        value += coef[7, t] * column_shift(here, 2)
        value += coef[8, t] * column_shift(here, -2)
        return value

    for t in range(STEPS):
        load = lambda i: field[X0, i]
        basis[0, t] = jnp.zeros((8, 256), jnp.float32)
        basis[1, t] = field[B, t] - SCALE * operate(load, t) - SHIFT * load(t)

    def grow(k, carry):
        for t in range(STEPS):
            load = lambda i: basis[k + 1, i]
            basis[k + 2, t] = operate(load, t) - BACK * basis[k, t]
        return carry

    lax.fori_loop(0, RESTART, grow, 0)

    size = 4
    for bi in range(VECTORS // size):
        for bj in range(bi + 1):
            pairs = [
                (i, j)
                for i in range(bi * size, bi * size + size)
                for j in range(bj * size, bj * size + size)
                if j <= i
            ]
            sums = {}
            for t in range(STEPS):
                need = sorted({i for pair in pairs for i in pair})
                cells = {i: basis[i + 1, t, :, 0:128] for i in need}
                for i, j in pairs:
                    product = cells[i] * cells[j]
                    sums[i, j] = product if t == 0 else sums[i, j] + product
            for i, j in pairs:
                total = jnp.sum(sums[i, j], axis=0, keepdims=True)
                gram_parts[i, j : j + 1, :] = total
                if i != j:
                    gram_parts[j, i : i + 1, :] = total

    place_in = lane - 32 * (row & 3)
    packed = jnp.zeros((8, 128), jnp.float32)
    for k in range(VECTORS):
        for half in range(2):
            total = jnp.sum(gram_parts[k, 8 * half : 8 * half + 8, :], axis=1, keepdims=True)
            packed = jnp.where(place_in == 2 * k + half, total, packed)
    for r in range(2):
        line = jnp.sum(packed[4 * r : 4 * r + 4, :], axis=0, keepdims=True)
        share[r : r + 1, :] = line
        gathered[me, r : r + 1, :] = line

    for o in range(1, devices):
        pltpu.make_async_remote_copy(
            share,
            gathered.at[me],
            send_sem,
            recv_sem,
            device_id=lax.rem(me + o, devices),
            device_id_type=LOGICAL,
        ).start()
    mirror_copy = pltpu.make_async_remote_copy(
        basis.at[pl.ds(1, VECTORS), :, :, pl.ds(0, 128)],
        mirror,
        mirror_sem.at[0],
        mirror_sem.at[1],
        device_id=sibling,
        device_id_type=pl.DeviceIdType.MESH,
    )
    mirror_copy.start()
    others = gathered.at[pl.ds(0, devices - 1)]
    everyone = pltpu.make_async_remote_copy(
        others, others, send_sem, recv_sem, device_id=sibling, device_id_type=pl.DeviceIdType.MESH
    )
    everyone.wait_recv()
    summed = jnp.sum(gathered[...], axis=0)
    summed = jnp.where(
        row < 4,
        jnp.broadcast_to(summed[0:1, :], (8, 128)),
        jnp.broadcast_to(summed[1:2, :], (8, 128)),
    )
    mirror_copy.wait()

    values = values_at_zero()
    columns = []
    for k in range(VECTORS):
        columns.append(
            [
                jnp.broadcast_to(
                    jnp.sum(
                        jnp.where(place_in == 2 * k + h, summed, 0.0), axis=1, keepdims=True
                    ),
                    (8, 128),
                )
                for h in range(2)
            ]
        )
    start = []
    for h in range(2):
        value = jnp.full((8, 128), values[8 * h], jnp.float32)
        for s in range(1, 8):
            value = jnp.where(row == s, values[8 * h + s], value)
        start.append(value)
    columns.append(list(start))

    def entry(column, i):
        return jnp.broadcast_to(column[i // 8][i % 8 : i % 8 + 1, :], (8, 128))

    for k in range(VECTORS):
        pivot = columns[k]
        inverse = 1.0 / entry(pivot, k)
        for j in range(k + 1, VECTORS + 1):
            factor = (entry(pivot, j) if j < VECTORS else entry(columns[j], k)) * inverse
            for h in range(2):
                columns[j][h] = columns[j][h] - pivot[h] * factor
            columns[j][k // 8] = jnp.where(row == k % 8, factor, columns[j][k // 8])
    u = columns[VECTORS]
    norm = jnp.sum(start[0] * u[0] + start[1] * u[1], axis=0, keepdims=True)
    inverse = jnp.broadcast_to(1.0 / norm, (8, 128))
    left_over = [entry(u, j) * inverse for j in range(VECTORS)]
    weights = [None] * RESTART
    for j in range(RESTART, 0, -1):
        value = left_over[j] * (-1.0 / SCALE)
        if j + 1 < RESTART:
            value = value - BACK * weights[j + 1]
        if j < RESTART:
            value = value - (SHIFT / SCALE) * weights[j]
        weights[j - 1] = value

    for t in range(STEPS):
        strided = pl.ds(t, 8, stride=STEPS)
        near = row < 4
        answer = jnp.where(
            near, block[X0, core, strided, :], pltpu.roll(block[X0, far, strided, :], 4, 0)
        )
        residual = jnp.zeros((8, 128), jnp.float32)
        for k in range(VECTORS):
            cells = jnp.where(near, basis[k + 1, t, :, 0:128], mirror[k, t])
            residual = residual + left_over[k] * cells
            if k < RESTART:
                answer = answer + weights[k] * cells
        out[0, strided, :] = answer
        out[1, strided, :] = residual

    stores = []
    for o in range(2):
        for part in range(2):
            tile = core if part == 0 else far
            copy = pltpu.make_async_copy(
                out.at[o, pl.ds(64 * part, 64), :],
                outputs[o].at[:, pl.ds(pl.multiple_of(128 * tile, 128), 128)],
                out_sem.at[o, part],
            )
            copy.start()
            stores.append(copy)
    everyone.wait_send()
    for copy in sends:
        copy.wait_send()
    for copy in stores:
        copy.wait()


def per_device(sizes, *arrays):
    devices = 1
    for a in AXES:
        devices *= sizes[a]
    f32 = jnp.float32
    dma = pltpu.SemaphoreType.DMA
    shape = jax.ShapeDtypeStruct((64, 256), f32)
    return pl.pallas_call(
        functools.partial(kernel, sizes),
        out_shape=(shape, shape),
        in_specs=[pl.BlockSpec(memory_space=pl.ANY)] * 5,
        out_specs=(pl.BlockSpec(memory_space=pl.ANY),) * 2,
        scratch_shapes=[
            pltpu.VMEM((5, 2, 128, 128), f32),
            pltpu.VMEM((2, 64, 128), f32),
            pltpu.VMEM((2, 128, 128), f32),
            pltpu.VMEM((9, STEPS, 8, 256), f32),
            pltpu.VMEM((5, STEPS, 8, 256), f32),
            pltpu.VMEM((VECTORS + 1, STEPS, 8, 256), f32),
            pltpu.VMEM((VECTORS, STEPS, 8, 128), f32),
            pltpu.VMEM((VECTORS, VECTORS, 128), f32),
            pltpu.VMEM((2, 128, 128), f32),
            pltpu.VMEM((devices, 2, 128), f32),
            pltpu.VMEM((2, 128), f32),
            dma((5, 2)),
            dma((2,)),
            dma((2, 2)),
            dma((2, 2)),
            dma((2,)),
            dma((2, 2)),
            dma,
            dma,
        ],
        compiler_params=pltpu.CompilerParams(collective_id=0, has_side_effects=True),
    )(*arrays)


def solution(mesh):
    counts = (4, 4, 4) if mesh.shape["gy"] == 64 else (1, 2, mesh.shape["gy"] // 2)
    torus = Mesh(mesh.devices.reshape((mesh.shape["gx"],) + counts), AXES)
    spec = P("gx", GY)
    return jax.shard_map(
        functools.partial(per_device, dict(torus.shape)),
        mesh=torus,
        in_specs=(spec,) * 5,
        out_specs=(spec, spec),
        check_vma=False,
    )
```

```python
import functools

import jax
import jax.numpy as jnp
from jax import lax
from jax.experimental import pallas as pl
from jax.experimental.pallas import tpu as pltpu
from jax.sharding import Mesh
from jax.sharding import PartitionSpec as P

RESTART = 15
VECTORS = RESTART + 1
GY = ("gy_0", "gy_1", "gy_2")
AXES = ("gx",) + GY
LOGICAL = pl.DeviceIdType.LOGICAL
DEPTH = 32
GROUPS = 4
STEPS = 16
SHIFT, SCALE = 5.525, 2.65
B, X0, RE, VX, VY = 0, 1, 2, 3, 4
PACKED = (X0, RE, VX, VY)


def values_at_zero():
    values = [1.0, -SHIFT / SCALE]
    for _ in range(VECTORS - 2):
        values.append(-(SHIFT / SCALE) * values[-1] - values[-2])
    return values


def kernel(sizes, *refs):
    inputs = refs[:5]
    out = refs[5]
    (block, pack, halo, halo_b, edge_b, coef, field, basis, merged, mirror, gram_parts) = refs[
        6:17
    ]
    (gathered, share) = refs[17:19]
    (load_sem, swap_sem, halo_send, halo_recv, mirror_sem, send_sem, recv_sem) = refs[19:]
    devices = 1
    for a in AXES:
        devices *= sizes[a]

    place = {a: lax.axis_index(a) for a in AXES}
    core = place["gx"]
    sibling = {"gx": 1 - core}

    def along(step):
        total = sizes["gy_0"] * sizes["gy_1"] * sizes["gy_2"]
        flat = (place["gy_0"] * sizes["gy_1"] + place["gy_1"]) * sizes["gy_2"] + place["gy_2"]
        flat = lax.rem(flat + step + total, total)
        low = lax.rem(flat, sizes["gy_2"])
        rest = lax.div(flat, sizes["gy_2"])
        return lax.div(rest, sizes["gy_1"]), lax.rem(rest, sizes["gy_1"]), low

    right, left = along(1), along(-1)

    def at(chip, core_index):
        return {"gx": core_index, "gy_0": chip[0], "gy_1": chip[1], "gy_2": chip[2]}

    me = core
    for a in GY:
        me = me * sizes[a] + place[a]

    loads = []
    for a in range(5):
        for tile in range(2):
            loads.append(
                pltpu.make_async_copy(
                    inputs[a].at[:, pl.ds(128 * tile, 128)],
                    block.at[a, tile, pl.ds(0, 64), :],
                    load_sem.at[a, tile],
                )
            )
            loads[-1].start()
    barrier = pltpu.get_barrier_semaphore()
    for o in range(1, devices):
        pl.semaphore_signal(
            barrier, inc=1, device_id=lax.bitwise_and(me + o, devices - 1), device_id_type=LOGICAL
        )
    for load in loads:
        load.wait()

    lane = lax.broadcasted_iota(jnp.int32, (8, 128), 1)
    row = lax.broadcasted_iota(jnp.int32, (8, 128), 0)

    for i in range(8):
        rows = pl.ds(8 * i, 8)
        for side, tile, first in ((0, 1, 96), (1, 0, 0)):
            value = block[PACKED[0], tile, rows, :]
            for g in range(1, GROUPS):
                start = (first + DEPTH * g) % 128
                moved = pltpu.roll(block[PACKED[g], tile, rows, :], DEPTH * g, 1)
                inside = (lane >= start) & (lane < start + DEPTH)
                value = jnp.where(inside, moved, value)
            pack[side, rows, :] = value
    for i in range(2):
        for side, tile, first in ((0, 1, 96), (1, 0, 0)):
            value = block[B, tile, pl.ds(8 * i, 8), :]
            for g in range(1, GROUPS):
                start = (first + DEPTH * g) % 128
                moved = pltpu.roll(block[B, tile, pl.ds(16 * g + 8 * i, 8), :], DEPTH * g, 1)
                inside = (lane >= start) & (lane < start + DEPTH)
                value = jnp.where(inside, moved, value)
            pack[side, pl.ds(64 + 8 * i, 8), :] = value

    pl.semaphore_wait(barrier, devices - 1)

    swap = pltpu.make_async_remote_copy(
        block.at[:, :, pl.ds(0, 64), :],
        block.at[:, :, pl.ds(64, 64), :],
        swap_sem.at[0],
        swap_sem.at[1],
        device_id=sibling,
        device_id_type=pl.DeviceIdType.MESH,
    )
    swap.start()
    sends = []
    for side, chip, target in ((0, right, 0), (1, left, 1)):
        same = core if target == 0 else 1 - core
        for part in range(2):
            if part == 0:
                source = pack.at[side, pl.ds(0, 64), :]
                landing = halo.at[pl.ds(pl.multiple_of(64 * same, 64), 64), :]
            else:
                source = pack.at[side, pl.ds(64, 16), :]
                landing = halo_b.at[pl.ds(pl.multiple_of(16 * same, 16), 16), :]
            copy = pltpu.make_async_remote_copy(
                source,
                landing,
                halo_send.at[side, part],
                halo_recv.at[part, same],
                device_id=at(chip, target),
                device_id_type=pl.DeviceIdType.MESH,
            )
            copy.start()
            sends.append(copy)
    far = 1 - core
    inv = 1.0 / SCALE

    def row_shift(load, t):
        if t >= STEPS:
            return pltpu.roll(load(t - STEPS), 7, 0)
        if t < 0:
            return pltpu.roll(load(t + STEPS), 1, 0)
        return load(t)

    def column_shift(value, offset):
        return pltpu.roll(value, (-offset) % 128, 1)

    def build(q, first, edge):
        inside = (lane >= first) & (lane < first + DEPTH)
        for a in range(5):
            for t in range(STEPS):
                strided = pl.ds(t, 8, stride=STEPS)
                field[a, q, t] = jnp.where(inside, edge(a, strided), block[a, core, strided, :])
        for t in range(STEPS):
            speed = lambda i: field[VX, q, i]
            here = speed(t)
            coef[0, q, t] = (field[RE, q, t] + (5.0 - SHIFT)) * inv
            coef[1, q, t] = (here + row_shift(speed, t + 1)) * (inv / 3.0) - 4.0 / 3.0 * inv
            coef[2, q, t] = (here + row_shift(speed, t - 1)) * (-inv / 3.0) - 4.0 / 3.0 * inv
            coef[3, q, t] = (here + row_shift(speed, t + 2)) * (-inv / 24.0) + inv / 12.0
            coef[4, q, t] = (here + row_shift(speed, t - 2)) * (inv / 24.0) + inv / 12.0
            here = field[VY, q, t]
            coef[5, q, t] = (here + column_shift(here, 1)) * (inv / 3.0) - 4.0 / 3.0 * inv
            coef[6, q, t] = (here + column_shift(here, -1)) * (-inv / 3.0) - 4.0 / 3.0 * inv
            coef[7, q, t] = (here + column_shift(here, 2)) * (-inv / 24.0) + inv / 12.0
            coef[8, q, t] = (here + column_shift(here, -2)) * (inv / 24.0) + inv / 12.0

    swap.wait()
    build(1 - core, 96 * core, lambda a, strided: block[a, far, strided, :])

    for part, ref, count in ((0, halo, 64), (1, halo_b, 16)):
        for half in range(2):
            landing = ref.at[pl.ds(count * half, count), :]
            pltpu.make_async_remote_copy(
                landing,
                landing,
                halo_send.at[0, part],
                halo_recv.at[part, half],
                device_id=sibling,
                device_id_type=pl.DeviceIdType.MESH,
            ).wait_recv()
    for s in range(8):
        for i in range(2):
            value = halo_b[pl.ds(16 * (s // 4) + 8 * i, 8), :]
            if s % 4:
                value = pltpu.roll(value, 128 - DEPTH * (s % 4), 1)
            edge_b[pl.ds(16 * s + 8 * i, 8), :] = value

    def from_chip(a, strided):
        if a == B:
            return edge_b[strided, :]
        g = PACKED.index(a)
        edge = halo[strided, :]
        return pltpu.roll(edge, 128 - DEPTH * g, 1) if g else edge

    build(core, 96 * (1 - core), from_chip)

    def operate(load, q, t):
        here = load(t)
        value = coef[0, q, t] * here
        value += coef[1, q, t] * row_shift(load, t + 1)
        value += coef[2, q, t] * row_shift(load, t - 1)
        value += coef[3, q, t] * row_shift(load, t + 2)
        value += coef[4, q, t] * row_shift(load, t - 2)
        value += coef[5, q, t] * column_shift(here, 1)
        value += coef[6, q, t] * column_shift(here, -1)
        value += coef[7, q, t] * column_shift(here, 2)
        value += coef[8, q, t] * column_shift(here, -2)
        return value

    own_left = lane < 64
    for t in range(STEPS):
        parts = []
        for q in range(2):
            load = lambda i: field[X0, q, i]
            basis[0, q, t] = jnp.zeros((8, 128), jnp.float32)
            parts.append(field[B, q, t] - SCALE * operate(load, q, t) - SHIFT * load(t))
            basis[1, q, t] = parts[q]
        merged[0, t] = jnp.where(own_left, parts[0], parts[1])

    def grow(k, carry):
        for t in range(STEPS):
            parts = []
            for q in range(2):
                load = lambda i: basis[k + 1, q, i]
                parts.append(operate(load, q, t) - basis[k, q, t])
                basis[k + 2, q, t] = parts[q]
            merged[k + 1, t] = jnp.where(own_left, parts[0], parts[1])
        return carry

    lax.fori_loop(0, RESTART, grow, 0, unroll=RESTART)

    size = 4
    for bi in range(VECTORS // size):
        for bj in range(bi + 1):
            pairs = [
                (i, j)
                for i in range(bi * size, bi * size + size)
                for j in range(bj * size, bj * size + size)
                if j <= i
            ]
            sums = {}
            for t in range(STEPS):
                need = sorted({i for pair in pairs for i in pair})
                cells = {i: merged[i, t] for i in need}
                for i, j in pairs:
                    product = cells[i] * cells[j]
                    sums[i, j] = product if t == 0 else sums[i, j] + product
            for i, j in pairs:
                total = jnp.sum(sums[i, j], axis=0, keepdims=True)
                gram_parts[i, j : j + 1, :] = total
                if i != j:
                    gram_parts[j, i : i + 1, :] = total

    place_in = lane - 32 * (row & 3)
    packed = jnp.zeros((8, 128), jnp.float32)
    for k in range(VECTORS):
        for half in range(2):
            total = jnp.sum(gram_parts[k, 8 * half : 8 * half + 8, :], axis=1, keepdims=True)
            packed = jnp.where(place_in == 2 * k + half, total, packed)
    for r in range(2):
        line = jnp.sum(packed[4 * r : 4 * r + 4, :], axis=0, keepdims=True)
        share[r : r + 1, :] = line
        gathered[me, r : r + 1, :] = line

    for o in range(1, devices):
        pltpu.make_async_remote_copy(
            share,
            gathered.at[me],
            send_sem,
            recv_sem,
            device_id=lax.bitwise_and(me + o, devices - 1),
            device_id_type=LOGICAL,
        ).start()
    mirror_copy = pltpu.make_async_remote_copy(
        merged,
        mirror,
        mirror_sem.at[0],
        mirror_sem.at[1],
        device_id=sibling,
        device_id_type=pl.DeviceIdType.MESH,
    )
    mirror_copy.start()
    others = gathered.at[pl.ds(0, devices - 1)]
    everyone = pltpu.make_async_remote_copy(
        others, others, send_sem, recv_sem, device_id=sibling, device_id_type=pl.DeviceIdType.MESH
    )
    everyone.wait_recv()
    summed = jnp.sum(gathered[...], axis=0)
    summed = jnp.where(
        row < 4,
        jnp.broadcast_to(summed[0:1, :], (8, 128)),
        jnp.broadcast_to(summed[1:2, :], (8, 128)),
    )
    mirror_copy.wait()

    values = values_at_zero()
    columns = []
    for k in range(VECTORS):
        columns.append(
            [
                jnp.broadcast_to(
                    jnp.sum(
                        jnp.where(place_in == 2 * k + h, summed, 0.0), axis=1, keepdims=True
                    ),
                    (8, 128),
                )
                for h in range(2)
            ]
        )
    start = []
    for h in range(2):
        value = jnp.full((8, 128), values[8 * h], jnp.float32)
        for s in range(1, 8):
            value = jnp.where(row == s, values[8 * h + s], value)
        start.append(value)
    columns.append(list(start))

    def entry(column, i):
        return jnp.broadcast_to(column[i // 8][i % 8 : i % 8 + 1, :], (8, 128))

    for k in range(VECTORS):
        pivot = columns[k]
        inverse = 1.0 / entry(pivot, k)
        for j in range(k + 1, VECTORS + 1):
            factor = (entry(pivot, j) if j < VECTORS else entry(columns[j], k)) * inverse
            for h in range(2):
                columns[j][h] = columns[j][h] - pivot[h] * factor
            columns[j][k // 8] = jnp.where(row == k % 8, factor, columns[j][k // 8])
    u = columns[VECTORS]
    norm = jnp.sum(start[0] * u[0] + start[1] * u[1], axis=0, keepdims=True)
    inverse = jnp.broadcast_to(1.0 / norm, (8, 128))
    left_over = [entry(u, j) * inverse for j in range(VECTORS)]
    weights = [None] * RESTART
    for j in range(RESTART, 0, -1):
        value = left_over[j] * (-1.0 / SCALE)
        if j + 1 < RESTART:
            value = value - weights[j + 1]
        if j < RESTART:
            value = value - (SHIFT / SCALE) * weights[j]
        weights[j - 1] = value

    for t in range(STEPS):
        strided = pl.ds(t, 8, stride=STEPS)
        near = row < 4
        answer = jnp.where(
            near, block[X0, core, strided, :], pltpu.roll(block[X0, far, strided, :], 4, 0)
        )
        residual = jnp.zeros((8, 128), jnp.float32)
        for k in range(VECTORS):
            cells = jnp.where(near, merged[k, t], mirror[k, t])
            residual = residual + left_over[k] * cells
            if k < RESTART:
                answer = answer + weights[k] * cells
        out[0, strided, :] = answer
        out[1, strided, :] = residual

    everyone.wait_send()
    for copy in sends:
        copy.wait_send()


def put_out(tiles, first, second, sem):
    core = lax.axis_index("gx")
    stores = []
    for o, output in enumerate((first, second)):
        for part in range(2):
            tile = core if part == 0 else 1 - core
            copy = pltpu.make_async_copy(
                tiles.at[o, pl.ds(64 * part, 64), :],
                output.at[:, pl.ds(pl.multiple_of(128 * tile, 128), 128)],
                sem.at[o, part],
            )
            copy.start()
            stores.append(copy)
    for copy in stores:
        copy.wait()


def per_device(sizes, *arrays):
    devices = 1
    for a in AXES:
        devices *= sizes[a]
    f32 = jnp.float32
    dma = pltpu.SemaphoreType.DMA
    shape = jax.ShapeDtypeStruct((64, 256), f32)
    tiles = pl.pallas_call(
        functools.partial(kernel, sizes),
        out_shape=pltpu.VMEM((2, 128, 128), f32),
        in_specs=[pl.BlockSpec(memory_space=pl.ANY)] * 5,
        out_specs=pl.BlockSpec(memory_space=pltpu.VMEM),
        scratch_shapes=[
            pltpu.VMEM((5, 2, 128, 128), f32),
            pltpu.VMEM((2, 80, 128), f32),
            pltpu.VMEM((128, 128), f32),
            pltpu.VMEM((32, 128), f32),
            pltpu.VMEM((128, 128), f32),
            pltpu.VMEM((9, 2, STEPS, 8, 128), f32),
            pltpu.VMEM((5, 2, STEPS, 8, 128), f32),
            pltpu.VMEM((VECTORS + 1, 2, STEPS, 8, 128), f32),
            pltpu.VMEM((VECTORS, STEPS, 8, 128), f32),
            pltpu.VMEM((VECTORS, STEPS, 8, 128), f32),
            pltpu.VMEM((VECTORS, VECTORS, 128), f32),
            pltpu.VMEM((devices, 2, 128), f32),
            pltpu.VMEM((2, 128), f32),
            dma((5, 2)),
            dma((2,)),
            dma((2, 2)),
            dma((2, 2)),
            dma((2,)),
            dma,
            dma,
        ],
        compiler_params=pltpu.CompilerParams(collective_id=0, has_side_effects=True),
    )(*arrays)
    return pl.pallas_call(
        put_out,
        out_shape=(shape, shape),
        in_specs=[pl.BlockSpec(memory_space=pltpu.VMEM)],
        out_specs=(pl.BlockSpec(memory_space=pl.ANY),) * 2,
        scratch_shapes=[dma((2, 2))],
    )(pltpu.with_memory_space_constraint(tiles, pltpu.VMEM))


def solution(mesh):
    counts = (4, 4, 4) if mesh.shape["gy"] == 64 else (1, 2, mesh.shape["gy"] // 2)
    torus = Mesh(mesh.devices.reshape((mesh.shape["gx"],) + counts), AXES)
    spec = P("gx", GY)
    return jax.shard_map(
        functools.partial(per_device, dict(torus.shape)),
        mesh=torus,
        in_specs=(spec,) * 5,
        out_specs=(spec, spec),
        check_vma=False,
    )
```

```python
import functools
import itertools

import jax
import jax.numpy as jnp
from jax import lax
from jax.experimental import pallas as pl
from jax.experimental.pallas import tpu as pltpu
from jax.sharding import Mesh
from jax.sharding import PartitionSpec as P

RESTART = 15
VECTORS = RESTART + 1
GY = ("gy_0", "gy_1", "gy_2")
AXES = ("gx",) + GY
LOGICAL = pl.DeviceIdType.LOGICAL
DEPTH = 32
GROUPS = 4
STEPS = 16
SHIFT, SCALE = 5.525, 2.65
B, X0, RE, VX, VY = 0, 1, 2, 3, 4
PACKED = (X0, RE, VX, VY)


def values_at_zero():
    values = [1.0, -SHIFT / SCALE]
    for _ in range(VECTORS - 2):
        values.append(-(SHIFT / SCALE) * values[-1] - values[-2])
    return values


def kernel(sizes, *refs):
    inputs = refs[:5]
    out = refs[5]
    (block, pack, halo, halo_b, edge_b, coef, field, basis, merged, mirror, gram_parts) = refs[
        6:17
    ]
    (gathered, share) = refs[17:19]
    (load_sem, swap_sem, halo_send, halo_recv, mirror_sem, send_sem, recv_sem, round_sem) = refs[19:]
    devices = 1
    for a in AXES:
        devices *= sizes[a]

    place = {a: lax.axis_index(a) for a in AXES}
    core = place["gx"]
    sibling = {"gx": 1 - core}

    def along(step):
        total = sizes["gy_0"] * sizes["gy_1"] * sizes["gy_2"]
        flat = (place["gy_0"] * sizes["gy_1"] + place["gy_1"]) * sizes["gy_2"] + place["gy_2"]
        flat = lax.rem(flat + step + total, total)
        low = lax.rem(flat, sizes["gy_2"])
        rest = lax.div(flat, sizes["gy_2"])
        return lax.div(rest, sizes["gy_1"]), lax.rem(rest, sizes["gy_1"]), low

    right, left = along(1), along(-1)

    def at(chip, core_index):
        return {"gx": core_index, "gy_0": chip[0], "gy_1": chip[1], "gy_2": chip[2]}

    me = core
    for a in GY:
        me = me * sizes[a] + place[a]

    loads = []
    for a in range(5):
        for tile in range(2):
            loads.append(
                pltpu.make_async_copy(
                    inputs[a].at[:, pl.ds(128 * tile, 128)],
                    block.at[a, tile, pl.ds(0, 64), :],
                    load_sem.at[a, tile],
                )
            )
            loads[-1].start()
    barrier = pltpu.get_barrier_semaphore()
    peers = []
    for axes in (("gx", "gy_2"), ("gy_1",), ("gy_0",)):
        for offset in itertools.product(*[range(sizes[a]) for a in axes]):
            if any(offset):
                peers.append({a: lax.rem(place[a] + o, sizes[a]) for a, o in zip(axes, offset)})
    neighbours = [at(right, 0), at(right, 1), at(left, 0), at(left, 1)]

    def greet(devices_to, semaphore):
        for device in devices_to:
            pl.semaphore_signal(
                semaphore, inc=1, device_id=device, device_id_type=pl.DeviceIdType.MESH
            )

    greet(neighbours + peers, barrier)
    for load in loads:
        load.wait()

    lane = lax.broadcasted_iota(jnp.int32, (8, 128), 1)
    row = lax.broadcasted_iota(jnp.int32, (8, 128), 0)

    for i in range(8):
        rows = pl.ds(8 * i, 8)
        for side, tile, first in ((0, 1, 96), (1, 0, 0)):
            value = block[PACKED[0], tile, rows, :]
            for g in range(1, GROUPS):
                start = (first + DEPTH * g) % 128
                moved = pltpu.roll(block[PACKED[g], tile, rows, :], DEPTH * g, 1)
                inside = (lane >= start) & (lane < start + DEPTH)
                value = jnp.where(inside, moved, value)
            pack[side, rows, :] = value
    for i in range(2):
        for side, tile, first in ((0, 1, 96), (1, 0, 0)):
            value = block[B, tile, pl.ds(8 * i, 8), :]
            for g in range(1, GROUPS):
                start = (first + DEPTH * g) % 128
                moved = pltpu.roll(block[B, tile, pl.ds(16 * g + 8 * i, 8), :], DEPTH * g, 1)
                inside = (lane >= start) & (lane < start + DEPTH)
                value = jnp.where(inside, moved, value)
            pack[side, pl.ds(64 + 8 * i, 8), :] = value

    pl.semaphore_wait(barrier, len(neighbours) + len(peers))
    greet(peers, round_sem.at[0])

    swap = pltpu.make_async_remote_copy(
        block.at[:, :, pl.ds(0, 64), :],
        block.at[:, :, pl.ds(64, 64), :],
        swap_sem.at[0],
        swap_sem.at[1],
        device_id=sibling,
        device_id_type=pl.DeviceIdType.MESH,
    )
    swap.start()
    sends = []
    for side, chip, target in ((0, right, 0), (1, left, 1)):
        same = core if target == 0 else 1 - core
        for part in range(2):
            if part == 0:
                source = pack.at[side, pl.ds(0, 64), :]
                landing = halo.at[pl.ds(pl.multiple_of(64 * same, 64), 64), :]
            else:
                source = pack.at[side, pl.ds(64, 16), :]
                landing = halo_b.at[pl.ds(pl.multiple_of(16 * same, 16), 16), :]
            copy = pltpu.make_async_remote_copy(
                source,
                landing,
                halo_send.at[side, part],
                halo_recv.at[part, same],
                device_id=at(chip, target),
                device_id_type=pl.DeviceIdType.MESH,
            )
            copy.start()
            sends.append(copy)
    far = 1 - core
    inv = 1.0 / SCALE

    def row_shift(load, t):
        if t >= STEPS:
            return pltpu.roll(load(t - STEPS), 7, 0)
        if t < 0:
            return pltpu.roll(load(t + STEPS), 1, 0)
        return load(t)

    def column_shift(value, offset):
        return pltpu.roll(value, (-offset) % 128, 1)

    def build(q, first, edge):
        inside = (lane >= first) & (lane < first + DEPTH)
        for a in range(5):
            for t in range(STEPS):
                strided = pl.ds(t, 8, stride=STEPS)
                field[a, q, t] = jnp.where(inside, edge(a, strided), block[a, core, strided, :])
        for t in range(STEPS):
            speed = lambda i: field[VX, q, i]
            here = speed(t)
            coef[0, q, t] = (field[RE, q, t] + (5.0 - SHIFT)) * inv
            coef[1, q, t] = (here + row_shift(speed, t + 1)) * (inv / 3.0) - 4.0 / 3.0 * inv
            coef[2, q, t] = (here + row_shift(speed, t - 1)) * (-inv / 3.0) - 4.0 / 3.0 * inv
            coef[3, q, t] = (here + row_shift(speed, t + 2)) * (-inv / 24.0) + inv / 12.0
            coef[4, q, t] = (here + row_shift(speed, t - 2)) * (inv / 24.0) + inv / 12.0
            here = field[VY, q, t]
            coef[5, q, t] = (here + column_shift(here, 1)) * (inv / 3.0) - 4.0 / 3.0 * inv
            coef[6, q, t] = (here + column_shift(here, -1)) * (-inv / 3.0) - 4.0 / 3.0 * inv
            coef[7, q, t] = (here + column_shift(here, 2)) * (-inv / 24.0) + inv / 12.0
            coef[8, q, t] = (here + column_shift(here, -2)) * (inv / 24.0) + inv / 12.0

    swap.wait()
    build(1 - core, 96 * core, lambda a, strided: block[a, far, strided, :])
    pl.semaphore_wait(round_sem.at[0], len(peers))
    greet(peers, round_sem.at[1])

    for part, ref, count in ((0, halo, 64), (1, halo_b, 16)):
        for half in range(2):
            landing = ref.at[pl.ds(count * half, count), :]
            pltpu.make_async_remote_copy(
                landing,
                landing,
                halo_send.at[0, part],
                halo_recv.at[part, half],
                device_id=sibling,
                device_id_type=pl.DeviceIdType.MESH,
            ).wait_recv()
    for s in range(8):
        for i in range(2):
            value = halo_b[pl.ds(16 * (s // 4) + 8 * i, 8), :]
            if s % 4:
                value = pltpu.roll(value, 128 - DEPTH * (s % 4), 1)
            edge_b[pl.ds(16 * s + 8 * i, 8), :] = value

    def from_chip(a, strided):
        if a == B:
            return edge_b[strided, :]
        g = PACKED.index(a)
        edge = halo[strided, :]
        return pltpu.roll(edge, 128 - DEPTH * g, 1) if g else edge

    build(core, 96 * (1 - core), from_chip)

    def operate(load, q, t):
        here = load(t)
        value = coef[0, q, t] * here
        value += coef[1, q, t] * row_shift(load, t + 1)
        value += coef[2, q, t] * row_shift(load, t - 1)
        value += coef[3, q, t] * row_shift(load, t + 2)
        value += coef[4, q, t] * row_shift(load, t - 2)
        value += coef[5, q, t] * column_shift(here, 1)
        value += coef[6, q, t] * column_shift(here, -1)
        value += coef[7, q, t] * column_shift(here, 2)
        value += coef[8, q, t] * column_shift(here, -2)
        return value

    own_left = lane < 64
    for t in range(STEPS):
        parts = []
        for q in range(2):
            load = lambda i: field[X0, q, i]
            basis[0, q, t] = jnp.zeros((8, 128), jnp.float32)
            parts.append(field[B, q, t] - SCALE * operate(load, q, t) - SHIFT * load(t))
            basis[1, q, t] = parts[q]
        merged[0, t] = jnp.where(own_left, parts[0], parts[1])

    def grow(k, carry):
        for t in range(STEPS):
            parts = []
            for q in range(2):
                load = lambda i: basis[k + 1, q, i]
                parts.append(operate(load, q, t) - basis[k, q, t])
                basis[k + 2, q, t] = parts[q]
            merged[k + 1, t] = jnp.where(own_left, parts[0], parts[1])
        return carry

    lax.fori_loop(0, RESTART, grow, 0, unroll=RESTART)

    size = 4
    for bi in range(VECTORS // size):
        for bj in range(bi + 1):
            pairs = [
                (i, j)
                for i in range(bi * size, bi * size + size)
                for j in range(bj * size, bj * size + size)
                if j <= i
            ]
            sums = {}
            for t in range(STEPS):
                need = sorted({i for pair in pairs for i in pair})
                cells = {i: merged[i, t] for i in need}
                for i, j in pairs:
                    product = cells[i] * cells[j]
                    sums[i, j] = product if t == 0 else sums[i, j] + product
            for i, j in pairs:
                total = jnp.sum(sums[i, j], axis=0, keepdims=True)
                gram_parts[i, j : j + 1, :] = total
                if i != j:
                    gram_parts[j, i : i + 1, :] = total

    place_in = lane - 32 * (row & 3)
    packed = jnp.zeros((8, 128), jnp.float32)
    for k in range(VECTORS):
        for half in range(2):
            total = jnp.sum(gram_parts[k, 8 * half : 8 * half + 8, :], axis=1, keepdims=True)
            packed = jnp.where(place_in == 2 * k + half, total, packed)
    for r in range(2):
        line = jnp.sum(packed[4 * r : 4 * r + 4, :], axis=0, keepdims=True)
        share[r : r + 1, :] = line
        gathered[me, r : r + 1, :] = line

    pl.semaphore_wait(round_sem.at[1], len(peers))

    for o in range(1, devices):
        pltpu.make_async_remote_copy(
            share,
            gathered.at[me],
            send_sem,
            recv_sem,
            device_id=lax.bitwise_and(me + o, devices - 1),
            device_id_type=LOGICAL,
        ).start()
    mirror_copy = pltpu.make_async_remote_copy(
        merged,
        mirror,
        mirror_sem.at[0],
        mirror_sem.at[1],
        device_id=sibling,
        device_id_type=pl.DeviceIdType.MESH,
    )
    mirror_copy.start()
    others = gathered.at[pl.ds(0, devices - 1)]
    everyone = pltpu.make_async_remote_copy(
        others, others, send_sem, recv_sem, device_id=sibling, device_id_type=pl.DeviceIdType.MESH
    )
    everyone.wait_recv()
    summed = jnp.sum(gathered[...], axis=0)
    summed = jnp.where(
        row < 4,
        jnp.broadcast_to(summed[0:1, :], (8, 128)),
        jnp.broadcast_to(summed[1:2, :], (8, 128)),
    )
    mirror_copy.wait()

    values = values_at_zero()
    columns = []
    for k in range(VECTORS):
        columns.append(
            [
                jnp.broadcast_to(
                    jnp.sum(
                        jnp.where(place_in == 2 * k + h, summed, 0.0), axis=1, keepdims=True
                    ),
                    (8, 128),
                )
                for h in range(2)
            ]
        )
    start = []
    for h in range(2):
        value = jnp.full((8, 128), values[8 * h], jnp.float32)
        for s in range(1, 8):
            value = jnp.where(row == s, values[8 * h + s], value)
        start.append(value)
    columns.append(list(start))

    def entry(column, i):
        return jnp.broadcast_to(column[i // 8][i % 8 : i % 8 + 1, :], (8, 128))

    for k in range(VECTORS):
        pivot = columns[k]
        inverse = 1.0 / entry(pivot, k)
        for j in range(k + 1, VECTORS + 1):
            factor = (entry(pivot, j) if j < VECTORS else entry(columns[j], k)) * inverse
            for h in range(2):
                columns[j][h] = columns[j][h] - pivot[h] * factor
            columns[j][k // 8] = jnp.where(row == k % 8, factor, columns[j][k // 8])
    u = columns[VECTORS]
    norm = jnp.sum(start[0] * u[0] + start[1] * u[1], axis=0, keepdims=True)
    inverse = jnp.broadcast_to(1.0 / norm, (8, 128))
    left_over = [entry(u, j) * inverse for j in range(VECTORS)]
    weights = [None] * RESTART
    for j in range(RESTART, 0, -1):
        value = left_over[j] * (-1.0 / SCALE)
        if j + 1 < RESTART:
            value = value - weights[j + 1]
        if j < RESTART:
            value = value - (SHIFT / SCALE) * weights[j]
        weights[j - 1] = value

    for t in range(STEPS):
        strided = pl.ds(t, 8, stride=STEPS)
        near = row < 4
        answer = jnp.where(
            near, block[X0, core, strided, :], pltpu.roll(block[X0, far, strided, :], 4, 0)
        )
        residual = jnp.zeros((8, 128), jnp.float32)
        for k in range(VECTORS):
            cells = jnp.where(near, merged[k, t], mirror[k, t])
            residual = residual + left_over[k] * cells
            if k < RESTART:
                answer = answer + weights[k] * cells
        out[0, strided, :] = answer
        out[1, strided, :] = residual

    everyone.wait_send()
    for copy in sends:
        copy.wait_send()


def put_out(tiles, first, second, sem):
    core = lax.axis_index("gx")
    stores = []
    for o, output in enumerate((first, second)):
        for part in range(2):
            tile = core if part == 0 else 1 - core
            copy = pltpu.make_async_copy(
                tiles.at[o, pl.ds(64 * part, 64), :],
                output.at[:, pl.ds(pl.multiple_of(128 * tile, 128), 128)],
                sem.at[o, part],
            )
            copy.start()
            stores.append(copy)
    for copy in stores:
        copy.wait()


def per_device(sizes, *arrays):
    devices = 1
    for a in AXES:
        devices *= sizes[a]
    f32 = jnp.float32
    dma = pltpu.SemaphoreType.DMA
    shape = jax.ShapeDtypeStruct((64, 256), f32)
    tiles = pl.pallas_call(
        functools.partial(kernel, sizes),
        out_shape=pltpu.VMEM((2, 128, 128), f32),
        in_specs=[pl.BlockSpec(memory_space=pl.ANY)] * 5,
        out_specs=pl.BlockSpec(memory_space=pltpu.VMEM),
        scratch_shapes=[
            pltpu.VMEM((5, 2, 128, 128), f32),
            pltpu.VMEM((2, 80, 128), f32),
            pltpu.VMEM((128, 128), f32),
            pltpu.VMEM((32, 128), f32),
            pltpu.VMEM((128, 128), f32),
            pltpu.VMEM((9, 2, STEPS, 8, 128), f32),
            pltpu.VMEM((5, 2, STEPS, 8, 128), f32),
            pltpu.VMEM((VECTORS + 1, 2, STEPS, 8, 128), f32),
            pltpu.VMEM((VECTORS, STEPS, 8, 128), f32),
            pltpu.VMEM((VECTORS, STEPS, 8, 128), f32),
            pltpu.VMEM((VECTORS, VECTORS, 128), f32),
            pltpu.VMEM((devices, 2, 128), f32),
            pltpu.VMEM((2, 128), f32),
            dma((5, 2)),
            dma((2,)),
            dma((2, 2)),
            dma((2, 2)),
            dma((2,)),
            dma,
            dma,
            pltpu.SemaphoreType.REGULAR((2,)),
        ],
        compiler_params=pltpu.CompilerParams(collective_id=0, has_side_effects=True),
    )(*arrays)
    return pl.pallas_call(
        put_out,
        out_shape=(shape, shape),
        in_specs=[pl.BlockSpec(memory_space=pltpu.VMEM)],
        out_specs=(pl.BlockSpec(memory_space=pl.ANY),) * 2,
        scratch_shapes=[dma((2, 2))],
    )(pltpu.with_memory_space_constraint(tiles, pltpu.VMEM))


def solution(mesh):
    counts = (4, 4, 4) if mesh.shape["gy"] == 64 else (1, 2, mesh.shape["gy"] // 2)
    torus = Mesh(mesh.devices.reshape((mesh.shape["gx"],) + counts), AXES)
    spec = P("gx", GY)
    return jax.shard_map(
        functools.partial(per_device, dict(torus.shape)),
        mesh=torus,
        in_specs=(spec,) * 5,
        out_specs=(spec, spec),
        check_vma=False,
    )
```

```python
import functools
import itertools

import jax
import jax.numpy as jnp
from jax import lax
from jax.experimental import pallas as pl
from jax.experimental.pallas import tpu as pltpu
from jax.sharding import Mesh
from jax.sharding import PartitionSpec as P

RESTART = 15
VECTORS = RESTART + 1
GY = ("gy_0", "gy_1", "gy_2")
AXES = ("gx",) + GY
LOGICAL = pl.DeviceIdType.LOGICAL
DEPTH = 32
GROUPS = 4
STEPS = 16
SHIFT, SCALE = 5.525, 2.65
B, X0, RE, VX, VY = 0, 1, 2, 3, 4
PACKED = (X0, RE, VX, VY)


def values_at_zero():
    values = [1.0, -SHIFT / SCALE]
    for _ in range(VECTORS - 2):
        values.append(-(SHIFT / SCALE) * values[-1] - values[-2])
    return values


def kernel(sizes, *refs):
    inputs = refs[:5]
    out = refs[5]
    (block, pack_r, pack_l, halo_r, halo_rb, halo_l, halo_lb, edge_b) = refs[6:14]
    (coef, field, basis, merged, mirror, joined, gram_parts) = refs[14:21]
    (gathered, share) = refs[21:23]
    (load_sem, swap_sem, right_send, right_recv, left_send, left_recv) = refs[23:29]
    (mirror_sem, tail_sem, send_sem, recv_sem, round_sem) = refs[29:]
    devices = 1
    for a in AXES:
        devices *= sizes[a]

    place = {a: lax.axis_index(a) for a in AXES}
    core = place["gx"]
    far = 1 - core
    sibling = {"gx": far}

    def along(step):
        total = sizes["gy_0"] * sizes["gy_1"] * sizes["gy_2"]
        flat = (place["gy_0"] * sizes["gy_1"] + place["gy_1"]) * sizes["gy_2"] + place["gy_2"]
        flat = lax.rem(flat + step + total, total)
        low = lax.rem(flat, sizes["gy_2"])
        rest = lax.div(flat, sizes["gy_2"])
        return lax.div(rest, sizes["gy_1"]), lax.rem(rest, sizes["gy_1"]), low

    right, left = along(1), along(-1)

    def at(chip, core_index):
        return {"gx": core_index, "gy_0": chip[0], "gy_1": chip[1], "gy_2": chip[2]}

    me = core
    for a in GY:
        me = me * sizes[a] + place[a]

    loads = []
    for a in range(5):
        for tile in range(2):
            loads.append(
                pltpu.make_async_copy(
                    inputs[a].at[:, pl.ds(128 * tile, 128)],
                    block.at[a, tile, pl.ds(0, 64), :],
                    load_sem.at[a, tile],
                )
            )
            loads[-1].start()
    barrier = pltpu.get_barrier_semaphore()
    peers = []
    for axes in (("gx", "gy_2"), ("gy_1",), ("gy_0",)):
        for offset in itertools.product(*[range(sizes[a]) for a in axes]):
            if any(offset):
                peers.append({a: lax.rem(place[a] + o, sizes[a]) for a, o in zip(axes, offset)})
    neighbours = [at(right, 0), at(right, 1), at(left, 0), at(left, 1)]

    def greet(devices_to, semaphore):
        for device in devices_to:
            pl.semaphore_signal(
                semaphore, inc=1, device_id=device, device_id_type=pl.DeviceIdType.MESH
            )

    greet(neighbours + peers, barrier)
    for load in loads:
        load.wait()

    lane = lax.broadcasted_iota(jnp.int32, (8, 128), 1)
    row = lax.broadcasted_iota(jnp.int32, (8, 128), 0)

    for n, (first, second) in enumerate(((X0, RE), (VX, VY), (B, B))):
        count = 64 if first != B else 32
        for i in range(count // 8):
            other = 8 * i if first != B else 32 + 8 * i
            pack_r[pl.ds(64 * n + 8 * i, 8), :] = jnp.where(
                lane >= 64,
                block[first, 1, pl.ds(8 * i, 8), :],
                pltpu.roll(block[second, 1, pl.ds(other, 8), :], 64, 1),
            )

    def pack_left(place_at, piece):
        value = piece(0)
        for g in range(1, GROUPS):
            inside = (lane >= DEPTH * g) & (lane < DEPTH * (g + 1))
            value = jnp.where(inside, pltpu.roll(piece(g), DEPTH * g, 1), value)
        pack_l[pl.ds(place_at, 8), :] = value

    for i in range(8):
        pack_left(8 * i, lambda g: block[PACKED[g], 0, pl.ds(8 * i, 8), :])
    for i in range(2):
        pack_left(64 + 8 * i, lambda g: block[B, 0, pl.ds(16 * g + 8 * i, 8), :])

    pl.semaphore_wait(barrier, len(neighbours) + len(peers))
    greet(peers, round_sem.at[0])

    sends = []
    for n in range(3):
        count = 64 if n < 2 else 32
        rows = pl.ds(pl.multiple_of(count * core, count), count)
        sends.append(
            pltpu.make_async_remote_copy(
                pack_r.at[pl.ds(64 * n, count), :],
                halo_r.at[n, rows, :] if n < 2 else halo_rb.at[rows, :],
                right_send.at[n],
                right_recv.at[n, core],
                device_id=at(right, 0),
                device_id_type=pl.DeviceIdType.MESH,
            )
        )
        sends[-1].start()
    swap = pltpu.make_async_remote_copy(
        block.at[:, :, pl.ds(0, 64), :],
        block.at[:, :, pl.ds(64, 64), :],
        swap_sem.at[0],
        swap_sem.at[1],
        device_id=sibling,
        device_id_type=pl.DeviceIdType.MESH,
    )
    swap.start()
    for n in range(2):
        count = 64 if n == 0 else 16
        rows = pl.ds(pl.multiple_of(count * far, count), count)
        sends.append(
            pltpu.make_async_remote_copy(
                pack_l.at[pl.ds(64 * n, count), :],
                halo_l.at[rows, :] if n == 0 else halo_lb.at[rows, :],
                left_send.at[n],
                left_recv.at[n, far],
                device_id=at(left, 1),
                device_id_type=pl.DeviceIdType.MESH,
            )
        )
        sends[-1].start()

    def arrived(landing, sem):
        pltpu.make_async_remote_copy(
            landing,
            landing,
            sem,
            sem,
            device_id=sibling,
            device_id_type=pl.DeviceIdType.MESH,
        ).wait_recv()

    inv = 1.0 / SCALE

    def row_shift(load, t):
        if t >= STEPS:
            return pltpu.roll(load(t - STEPS), 7, 0)
        if t < 0:
            return pltpu.roll(load(t + STEPS), 1, 0)
        return load(t)

    def column_shift(value, offset):
        return pltpu.roll(value, (-offset) % 128, 1)

    def fill(q, inside, edge):
        for a in range(5):
            for t in range(STEPS):
                strided = pl.ds(t, 8, stride=STEPS)
                value = block[a, core, strided, :]
                if inside is not None:
                    value = jnp.where(inside, edge(a, strided), value)
                field[a, q, t] = value

    def build(q):
        for t in range(STEPS):
            speed = lambda i: field[VX, q, i]
            here = speed(t)
            coef[0, q, t] = (field[RE, q, t] + (5.0 - SHIFT)) * inv
            coef[1, q, t] = (here + row_shift(speed, t + 1)) * (inv / 3.0) - 4.0 / 3.0 * inv
            coef[2, q, t] = (here + row_shift(speed, t - 1)) * (-inv / 3.0) - 4.0 / 3.0 * inv
            coef[3, q, t] = (here + row_shift(speed, t + 2)) * (-inv / 24.0) + inv / 12.0
            coef[4, q, t] = (here + row_shift(speed, t - 2)) * (inv / 24.0) + inv / 12.0
            here = field[VY, q, t]
            coef[5, q, t] = (here + column_shift(here, 1)) * (inv / 3.0) - 4.0 / 3.0 * inv
            coef[6, q, t] = (here + column_shift(here, -1)) * (-inv / 3.0) - 4.0 / 3.0 * inv
            coef[7, q, t] = (here + column_shift(here, 2)) * (-inv / 24.0) + inv / 12.0
            coef[8, q, t] = (here + column_shift(here, -2)) * (inv / 24.0) + inv / 12.0

    swap.wait()
    fill(1, None, None)
    build(1)
    pl.semaphore_wait(round_sem.at[0], len(peers))
    greet(peers, round_sem.at[1])

    @pl.when(core == 1)
    def _():
        fill(0, lane >= 64, lambda a, strided: block[a, 0, strided, :])

    @pl.when(core == 0)
    def _():
        for n in range(3):
            for half in range(2):
                if n < 2:
                    arrived(halo_r.at[n, pl.ds(64 * half, 64), :], right_recv.at[n, half])
                else:
                    arrived(halo_rb.at[pl.ds(32 * half, 32), :], right_recv.at[n, half])
        for s in range(8):
            for i in range(2):
                value = halo_rb[pl.ds(32 * (s // 4) + 16 * (s % 2) + 8 * i, 8), :]
                if s % 4 >= 2:
                    value = pltpu.roll(value, 64, 1)
                edge_b[pl.ds(16 * s + 8 * i, 8), :] = value

        def from_left(a, strided):
            if a == B:
                return edge_b[strided, :]
            edge = halo_r[0 if a in (X0, RE) else 1, strided, :]
            return edge if a in (X0, VX) else pltpu.roll(edge, 64, 1)

        fill(0, lane >= 64, from_left)

    build(0)

    def operate(load, q, t):
        here = load(t)
        value = coef[0, q, t] * here
        value += coef[1, q, t] * row_shift(load, t + 1)
        value += coef[2, q, t] * row_shift(load, t - 1)
        value += coef[3, q, t] * row_shift(load, t + 2)
        value += coef[4, q, t] * row_shift(load, t - 2)
        value += coef[5, q, t] * column_shift(here, 1)
        value += coef[6, q, t] * column_shift(here, -1)
        value += coef[7, q, t] * column_shift(here, 2)
        value += coef[8, q, t] * column_shift(here, -2)
        return value

    middle = (lane >= 32) & (lane < 96)
    for t in range(STEPS):
        parts = []
        for q in range(2):
            load = lambda i: field[X0, q, i]
            basis[0, q, t] = jnp.zeros((8, 128), jnp.float32)
            parts.append(field[B, q, t] - SCALE * operate(load, q, t) - SHIFT * load(t))
            basis[1, q, t] = parts[q]
        merged[0, t] = jnp.where(middle, parts[1], parts[0])

    def grow(k, carry):
        for t in range(STEPS):
            parts = []
            for q in range(2):
                load = lambda i: basis[k + 1, q, i]
                parts.append(operate(load, q, t) - basis[k, q, t])
                basis[k + 2, q, t] = parts[q]
            merged[k + 1, t] = jnp.where(middle, parts[1], parts[0])
        return carry

    lax.fori_loop(0, RESTART, grow, 0, unroll=RESTART)

    size = 4
    for bi in range(VECTORS // size):
        for bj in range(bi + 1):
            pairs = [
                (i, j)
                for i in range(bi * size, bi * size + size)
                for j in range(bj * size, bj * size + size)
                if j <= i
            ]
            sums = {}
            for t in range(STEPS):
                need = sorted({i for pair in pairs for i in pair})
                cells = {i: merged[i, t] for i in need}
                for i, j in pairs:
                    product = cells[i] * cells[j]
                    sums[i, j] = product if t == 0 else sums[i, j] + product
            for i, j in pairs:
                total = jnp.sum(sums[i, j], axis=0, keepdims=True)
                gram_parts[i, j : j + 1, :] = total
                if i != j:
                    gram_parts[j, i : i + 1, :] = total

    place_in = lane - 32 * (row & 3)
    packed = jnp.zeros((8, 128), jnp.float32)
    for k in range(VECTORS):
        for half in range(2):
            total = jnp.sum(gram_parts[k, 8 * half : 8 * half + 8, :], axis=1, keepdims=True)
            packed = jnp.where(place_in == 2 * k + half, total, packed)
    for r in range(2):
        line = jnp.sum(packed[4 * r : 4 * r + 4, :], axis=0, keepdims=True)
        share[r : r + 1, :] = line
        gathered[me, r : r + 1, :] = line

    pl.semaphore_wait(round_sem.at[1], len(peers))

    for o in range(1, devices):
        pltpu.make_async_remote_copy(
            share,
            gathered.at[me],
            send_sem,
            recv_sem,
            device_id=lax.bitwise_and(me + o, devices - 1),
            device_id_type=LOGICAL,
        ).start()
    mirror_copy = pltpu.make_async_remote_copy(
        merged,
        mirror,
        mirror_sem.at[0],
        mirror_sem.at[1],
        device_id=sibling,
        device_id_type=pl.DeviceIdType.MESH,
    )
    mirror_copy.start()

    tail = basis.at[pl.ds(1, VECTORS), 2]
    tail_copy = pltpu.make_async_remote_copy(
        tail,
        tail,
        tail_sem.at[0],
        tail_sem.at[1],
        device_id=sibling,
        device_id_type=pl.DeviceIdType.MESH,
    )

    @pl.when(core == 1)
    def _():
        for n in range(2):
            for half in range(2):
                if n == 0:
                    arrived(halo_l.at[pl.ds(64 * half, 64), :], left_recv.at[n, half])
                else:
                    arrived(halo_lb.at[pl.ds(16 * half, 16), :], left_recv.at[n, half])
        for s in range(8):
            for i in range(2):
                value = halo_lb[pl.ds(16 * (s // 4) + 8 * i, 8), :]
                if s % 4:
                    value = pltpu.roll(value, 128 - DEPTH * (s % 4), 1)
                edge_b[pl.ds(16 * s + 8 * i, 8), :] = value

        def from_right(a, strided):
            if a == B:
                return edge_b[strided, :]
            g = PACKED.index(a)
            edge = halo_l[strided, :]
            return pltpu.roll(edge, 128 - DEPTH * g, 1) if g else edge

        fill(2, lane < DEPTH, from_right)
        build(2)
        for t in range(STEPS):
            load = lambda i: field[X0, 2, i]
            basis[0, 2, t] = jnp.zeros((8, 128), jnp.float32)
            basis[1, 2, t] = field[B, 2, t] - SCALE * operate(load, 2, t) - SHIFT * load(t)

        def grow_tail(k, carry):
            for t in range(STEPS):
                load = lambda i: basis[k + 1, 2, i]
                basis[k + 2, 2, t] = operate(load, 2, t) - basis[k, 2, t]
            return carry

        lax.fori_loop(0, RESTART, grow_tail, 0, unroll=3)
        tail_copy.start()

    mirror_copy.wait()

    @pl.when(core == 0)
    def _():
        tail_copy.wait_recv()

    upper = lane < 96
    near = row < 4
    is_first = (row * 0 + core) == 0
    in_first = near == is_first
    for k in range(VECTORS):
        for t in range(STEPS):
            own, other = merged[k, t], mirror[k, t]
            second = pltpu.roll(jnp.where(is_first, other, own), 4, 0)
            last = jnp.where(in_first, second, basis[k + 1, 2, t])
            joined[k, t] = jnp.where(upper, jnp.where(near, own, other), last)

    others = gathered.at[pl.ds(0, devices - 1)]
    everyone = pltpu.make_async_remote_copy(
        others, others, send_sem, recv_sem, device_id=sibling, device_id_type=pl.DeviceIdType.MESH
    )
    everyone.wait_recv()
    summed = jnp.sum(gathered[...], axis=0)
    summed = jnp.where(
        row < 4,
        jnp.broadcast_to(summed[0:1, :], (8, 128)),
        jnp.broadcast_to(summed[1:2, :], (8, 128)),
    )

    values = values_at_zero()
    columns = []
    for k in range(VECTORS):
        columns.append(
            [
                jnp.broadcast_to(
                    jnp.sum(
                        jnp.where(place_in == 2 * k + h, summed, 0.0), axis=1, keepdims=True
                    ),
                    (8, 128),
                )
                for h in range(2)
            ]
        )
    start = []
    for h in range(2):
        value = jnp.full((8, 128), values[8 * h], jnp.float32)
        for s in range(1, 8):
            value = jnp.where(row == s, values[8 * h + s], value)
        start.append(value)
    columns.append(list(start))

    def entry(column, i):
        return jnp.broadcast_to(column[i // 8][i % 8 : i % 8 + 1, :], (8, 128))

    for k in range(VECTORS):
        pivot = columns[k]
        inverse = 1.0 / entry(pivot, k)
        for j in range(k + 1, VECTORS + 1):
            factor = (entry(pivot, j) if j < VECTORS else entry(columns[j], k)) * inverse
            for h in range(2):
                columns[j][h] = columns[j][h] - pivot[h] * factor
            columns[j][k // 8] = jnp.where(row == k % 8, factor, columns[j][k // 8])
    u = columns[VECTORS]
    norm = jnp.sum(start[0] * u[0] + start[1] * u[1], axis=0, keepdims=True)
    inverse = jnp.broadcast_to(1.0 / norm, (8, 128))
    left_over = [entry(u, j) * inverse for j in range(VECTORS)]
    weights = [None] * RESTART
    for j in range(RESTART, 0, -1):
        value = left_over[j] * (-1.0 / SCALE)
        if j + 1 < RESTART:
            value = value - weights[j + 1]
        if j < RESTART:
            value = value - (SHIFT / SCALE) * weights[j]
        weights[j - 1] = value

    for t in range(STEPS):
        strided = pl.ds(t, 8, stride=STEPS)
        answer = jnp.where(
            near, block[X0, core, strided, :], pltpu.roll(block[X0, far, strided, :], 4, 0)
        )
        residual = jnp.zeros((8, 128), jnp.float32)
        for k in range(VECTORS):
            cells = joined[k, t]
            residual = residual + left_over[k] * cells
            if k < RESTART:
                answer = answer + weights[k] * cells
        out[0, strided, :] = answer
        out[1, strided, :] = residual

    everyone.wait_send()

    @pl.when(core == 1)
    def _():
        tail_copy.wait_send()

    for copy in sends:
        copy.wait_send()


def put_out(tiles, first, second, sem):
    core = lax.axis_index("gx")
    stores = []
    for o, output in enumerate((first, second)):
        for part in range(2):
            tile = core if part == 0 else 1 - core
            copy = pltpu.make_async_copy(
                tiles.at[o, pl.ds(64 * part, 64), :],
                output.at[:, pl.ds(pl.multiple_of(128 * tile, 128), 128)],
                sem.at[o, part],
            )
            copy.start()
            stores.append(copy)
    for copy in stores:
        copy.wait()


def per_device(sizes, *arrays):
    devices = 1
    for a in AXES:
        devices *= sizes[a]
    f32 = jnp.float32
    dma = pltpu.SemaphoreType.DMA
    shape = jax.ShapeDtypeStruct((64, 256), f32)
    tiles = pl.pallas_call(
        functools.partial(kernel, sizes),
        out_shape=pltpu.VMEM((2, 128, 128), f32),
        in_specs=[pl.BlockSpec(memory_space=pl.ANY)] * 5,
        out_specs=pl.BlockSpec(memory_space=pltpu.VMEM),
        scratch_shapes=[
            pltpu.VMEM((5, 2, 128, 128), f32),
            pltpu.VMEM((160, 128), f32),
            pltpu.VMEM((80, 128), f32),
            pltpu.VMEM((2, 128, 128), f32),
            pltpu.VMEM((64, 128), f32),
            pltpu.VMEM((128, 128), f32),
            pltpu.VMEM((32, 128), f32),
            pltpu.VMEM((128, 128), f32),
            pltpu.VMEM((9, 3, STEPS, 8, 128), f32),
            pltpu.VMEM((5, 3, STEPS, 8, 128), f32),
            pltpu.VMEM((VECTORS + 1, 3, STEPS, 8, 128), f32),
            pltpu.VMEM((VECTORS, STEPS, 8, 128), f32),
            pltpu.VMEM((VECTORS, STEPS, 8, 128), f32),
            pltpu.VMEM((VECTORS, STEPS, 8, 128), f32),
            pltpu.VMEM((VECTORS, VECTORS, 128), f32),
            pltpu.VMEM((devices, 2, 128), f32),
            pltpu.VMEM((2, 128), f32),
            dma((5, 2)),
            dma((2,)),
            dma((3,)),
            dma((3, 2)),
            dma((2,)),
            dma((2, 2)),
            dma((2,)),
            dma((2,)),
            dma,
            dma,
            pltpu.SemaphoreType.REGULAR((2,)),
        ],
        compiler_params=pltpu.CompilerParams(collective_id=0, has_side_effects=True),
    )(*arrays)
    return pl.pallas_call(
        put_out,
        out_shape=(shape, shape),
        in_specs=[pl.BlockSpec(memory_space=pltpu.VMEM)],
        out_specs=(pl.BlockSpec(memory_space=pl.ANY),) * 2,
        scratch_shapes=[dma((2, 2))],
    )(pltpu.with_memory_space_constraint(tiles, pltpu.VMEM))


def solution(mesh):
    counts = (4, 4, 4) if mesh.shape["gy"] == 64 else (1, 2, mesh.shape["gy"] // 2)
    torus = Mesh(mesh.devices.reshape((mesh.shape["gx"],) + counts), AXES)
    spec = P("gx", GY)
    return jax.shard_map(
        functools.partial(per_device, dict(torus.shape)),
        mesh=torus,
        in_specs=(spec,) * 5,
        out_specs=(spec, spec),
        check_vma=False,
    )
```

```python
import functools
import itertools

import jax
import jax.numpy as jnp
from jax import lax
from jax.experimental import pallas as pl
from jax.experimental.pallas import tpu as pltpu
from jax.sharding import Mesh
from jax.sharding import PartitionSpec as P

RESTART = 15
VECTORS = RESTART + 1
GY = ("gy_0", "gy_1", "gy_2")
AXES = ("gx",) + GY
LOGICAL = pl.DeviceIdType.LOGICAL
DEPTH = 32
GROUPS = 4
STEPS = 16
SHIFT, SCALE = 5.525, 2.65
B, X0, RE, VX, VY = 0, 1, 2, 3, 4
PACKED = (X0, RE, VX, VY)


def values_at_zero():
    values = [1.0, -SHIFT / SCALE]
    for _ in range(VECTORS - 2):
        values.append(-(SHIFT / SCALE) * values[-1] - values[-2])
    return values


def kernel(sizes, *refs):
    inputs = refs[:5]
    out = refs[5]
    (block, pack_r, pack_l, halo_r, halo_rb, halo_l, halo_lb, edge_b) = refs[6:14]
    (coef, field, basis, merged, mirror, joined, gram_parts) = refs[14:21]
    (gathered, share) = refs[21:23]
    (load_sem, swap_sem, right_send, right_recv, left_send, left_recv) = refs[23:29]
    (mirror_sem, tail_sem, send_sem, recv_sem, round_sem) = refs[29:]
    devices = 1
    for a in AXES:
        devices *= sizes[a]

    place = {a: lax.axis_index(a) for a in AXES}
    core = place["gx"]
    far = 1 - core
    sibling = {"gx": far}

    def along(step):
        total = sizes["gy_0"] * sizes["gy_1"] * sizes["gy_2"]
        flat = (place["gy_0"] * sizes["gy_1"] + place["gy_1"]) * sizes["gy_2"] + place["gy_2"]
        flat = lax.rem(flat + step + total, total)
        low = lax.rem(flat, sizes["gy_2"])
        rest = lax.div(flat, sizes["gy_2"])
        return lax.div(rest, sizes["gy_1"]), lax.rem(rest, sizes["gy_1"]), low

    right, left = along(1), along(-1)

    def at(chip, core_index):
        return {"gx": core_index, "gy_0": chip[0], "gy_1": chip[1], "gy_2": chip[2]}

    me = core
    for a in GY:
        me = me * sizes[a] + place[a]

    loads = []
    for a in range(5):
        for tile in range(2):
            loads.append(
                pltpu.make_async_copy(
                    inputs[a].at[:, pl.ds(128 * tile, 128)],
                    block.at[a, tile, pl.ds(0, 64), :],
                    load_sem.at[a, tile],
                )
            )
            loads[-1].start()
    barrier = pltpu.get_barrier_semaphore()
    peers = []
    for axes in (("gx", "gy_2"), ("gy_1",), ("gy_0",)):
        for offset in itertools.product(*[range(sizes[a]) for a in axes]):
            if any(offset):
                peers.append({a: lax.rem(place[a] + o, sizes[a]) for a, o in zip(axes, offset)})
    neighbours = [at(right, 0), at(right, 1), at(left, 0), at(left, 1)]

    def greet(devices_to, semaphore):
        for device in devices_to:
            pl.semaphore_signal(
                semaphore, inc=1, device_id=device, device_id_type=pl.DeviceIdType.MESH
            )

    greet(neighbours + peers, barrier)
    for load in loads:
        load.wait()

    lane = lax.broadcasted_iota(jnp.int32, (8, 128), 1)
    row = lax.broadcasted_iota(jnp.int32, (8, 128), 0)

    for n, (first, second) in enumerate(((X0, RE), (VX, VY), (B, B))):
        count = 64 if first != B else 32
        for i in range(count // 8):
            other = 8 * i if first != B else 32 + 8 * i
            pack_r[pl.ds(64 * n + 8 * i, 8), :] = jnp.where(
                lane >= 64,
                block[first, 1, pl.ds(8 * i, 8), :],
                pltpu.roll(block[second, 1, pl.ds(other, 8), :], 64, 1),
            )

    def pack_left(place_at, piece):
        value = piece(0)
        for g in range(1, GROUPS):
            inside = (lane >= DEPTH * g) & (lane < DEPTH * (g + 1))
            value = jnp.where(inside, pltpu.roll(piece(g), DEPTH * g, 1), value)
        pack_l[pl.ds(place_at, 8), :] = value

    for i in range(8):
        pack_left(8 * i, lambda g: block[PACKED[g], 0, pl.ds(8 * i, 8), :])
    for i in range(2):
        pack_left(64 + 8 * i, lambda g: block[B, 0, pl.ds(16 * g + 8 * i, 8), :])

    pl.semaphore_wait(barrier, len(neighbours) + len(peers))
    greet(peers, round_sem.at[0])

    sends = []
    for n in range(3):
        count = 64 if n < 2 else 32
        rows = pl.ds(pl.multiple_of(count * core, count), count)
        sends.append(
            pltpu.make_async_remote_copy(
                pack_r.at[pl.ds(64 * n, count), :],
                halo_r.at[n, rows, :] if n < 2 else halo_rb.at[rows, :],
                right_send.at[n],
                right_recv.at[n, core],
                device_id=at(right, 0),
                device_id_type=pl.DeviceIdType.MESH,
            )
        )
        sends[-1].start()
    swap = pltpu.make_async_remote_copy(
        block.at[:, :, pl.ds(0, 64), :],
        block.at[:, :, pl.ds(64, 64), :],
        swap_sem.at[0],
        swap_sem.at[1],
        device_id=sibling,
        device_id_type=pl.DeviceIdType.MESH,
    )
    swap.start()
    for n in range(2):
        count = 64 if n == 0 else 16
        rows = pl.ds(pl.multiple_of(count * far, count), count)
        sends.append(
            pltpu.make_async_remote_copy(
                pack_l.at[pl.ds(64 * n, count), :],
                halo_l.at[rows, :] if n == 0 else halo_lb.at[rows, :],
                left_send.at[n],
                left_recv.at[n, far],
                device_id=at(left, 1),
                device_id_type=pl.DeviceIdType.MESH,
            )
        )
        sends[-1].start()

    def arrived(landing, sem):
        pltpu.make_async_remote_copy(
            landing,
            landing,
            sem,
            sem,
            device_id=sibling,
            device_id_type=pl.DeviceIdType.MESH,
        ).wait_recv()

    inv = 1.0 / SCALE

    def row_shift(load, t):
        if t >= STEPS:
            return pltpu.roll(load(t - STEPS), 7, 0)
        if t < 0:
            return pltpu.roll(load(t + STEPS), 1, 0)
        return load(t)

    def column_shift(value, offset):
        return pltpu.roll(value, (-offset) % 128, 1)

    def fill(q, inside, edge):
        for a in range(5):
            for t in range(STEPS):
                strided = pl.ds(t, 8, stride=STEPS)
                value = block[a, core, strided, :]
                if inside is not None:
                    value = jnp.where(inside, edge(a, strided), value)
                field[a, q, t] = value

    def build(q):
        for t in range(STEPS):
            speed = lambda i: field[VX, q, i]
            here = speed(t)
            coef[0, q, t] = (field[RE, q, t] + (5.0 - SHIFT)) * inv
            coef[1, q, t] = (here + row_shift(speed, t + 1)) * (inv / 3.0) - 4.0 / 3.0 * inv
            coef[2, q, t] = (here + row_shift(speed, t - 1)) * (-inv / 3.0) - 4.0 / 3.0 * inv
            coef[3, q, t] = (here + row_shift(speed, t + 2)) * (-inv / 24.0) + inv / 12.0
            coef[4, q, t] = (here + row_shift(speed, t - 2)) * (inv / 24.0) + inv / 12.0
            here = field[VY, q, t]
            coef[5, q, t] = (here + column_shift(here, 1)) * (inv / 3.0) - 4.0 / 3.0 * inv
            coef[6, q, t] = (here + column_shift(here, -1)) * (-inv / 3.0) - 4.0 / 3.0 * inv
            coef[7, q, t] = (here + column_shift(here, 2)) * (-inv / 24.0) + inv / 12.0
            coef[8, q, t] = (here + column_shift(here, -2)) * (inv / 24.0) + inv / 12.0

    swap.wait()
    fill(1, None, None)
    build(1)
    pl.semaphore_wait(round_sem.at[0], len(peers))
    greet(peers, round_sem.at[1])

    @pl.when(core == 1)
    def _():
        fill(0, lane >= 64, lambda a, strided: block[a, 0, strided, :])

    @pl.when(core == 0)
    def _():
        for n in range(3):
            for half in range(2):
                if n < 2:
                    arrived(halo_r.at[n, pl.ds(64 * half, 64), :], right_recv.at[n, half])
                else:
                    arrived(halo_rb.at[pl.ds(32 * half, 32), :], right_recv.at[n, half])
        for s in range(8):
            for i in range(2):
                value = halo_rb[pl.ds(32 * (s // 4) + 16 * (s % 2) + 8 * i, 8), :]
                if s % 4 >= 2:
                    value = pltpu.roll(value, 64, 1)
                edge_b[pl.ds(16 * s + 8 * i, 8), :] = value

        def from_left(a, strided):
            if a == B:
                return edge_b[strided, :]
            edge = halo_r[0 if a in (X0, RE) else 1, strided, :]
            return edge if a in (X0, VX) else pltpu.roll(edge, 64, 1)

        fill(0, lane >= 64, from_left)

    build(0)

    def operate(load, q, t):
        here = load(t)
        value = coef[0, q, t] * here
        value += coef[1, q, t] * row_shift(load, t + 1)
        value += coef[2, q, t] * row_shift(load, t - 1)
        value += coef[3, q, t] * row_shift(load, t + 2)
        value += coef[4, q, t] * row_shift(load, t - 2)
        value += coef[5, q, t] * column_shift(here, 1)
        value += coef[6, q, t] * column_shift(here, -1)
        value += coef[7, q, t] * column_shift(here, 2)
        value += coef[8, q, t] * column_shift(here, -2)
        return value

    middle = (lane >= 32) & (lane < 96)
    for t in range(STEPS):
        parts = []
        for q in range(2):
            load = lambda i: field[X0, q, i]
            basis[0, q, t] = jnp.zeros((8, 128), jnp.float32)
            parts.append(field[B, q, t] - SCALE * operate(load, q, t) - SHIFT * load(t))
            basis[1, q, t] = parts[q]
        merged[0, t] = jnp.where(middle, parts[1], parts[0])

    def gram_row(k, others):
        sums = [None] * len(others)
        for t in range(STEPS):
            cells = merged[k, t]
            for n, j in enumerate(others):
                product = cells * (cells if j == k else merged[j, t])
                sums[n] = product if t == 0 else sums[n] + product
        for n, j in enumerate(others):
            total = jnp.sum(sums[n], axis=0, keepdims=True)
            gram_parts[k, j : j + 1, :] = total
            if j != k:
                gram_parts[j, k : k + 1, :] = total

    for k in range(VECTORS):
        chunks = [list(range(j, min(j + 4, k + 1))) for j in range(0, k + 1, 4)]
        if k < RESTART:
            for t in range(STEPS):
                parts = []
                for q in range(2):
                    load = lambda i: basis[k + 1, q, i]
                    parts.append(operate(load, q, t) - basis[k, q, t])
                    basis[k + 2, q, t] = parts[q]
                merged[k + 1, t] = jnp.where(middle, parts[1], parts[0])
                if t % 4 == 3 and chunks:
                    gram_row(k, chunks.pop(0))
        for chunk in chunks:
            gram_row(k, chunk)

    place_in = lane - 32 * (row & 3)
    packed = jnp.zeros((8, 128), jnp.float32)
    for k in range(VECTORS):
        for half in range(2):
            total = jnp.sum(gram_parts[k, 8 * half : 8 * half + 8, :], axis=1, keepdims=True)
            packed = jnp.where(place_in == 2 * k + half, total, packed)
    for r in range(2):
        line = jnp.sum(packed[4 * r : 4 * r + 4, :], axis=0, keepdims=True)
        share[r : r + 1, :] = line
        gathered[me, r : r + 1, :] = line

    pl.semaphore_wait(round_sem.at[1], len(peers))

    half = devices // 2
    mine = lax.rem(me, half) * 2 + core
    for o in range(devices - 1):
        chip = o + jnp.where(mine <= o, 1, 0)
        pltpu.make_async_remote_copy(
            share,
            gathered.at[me],
            send_sem,
            recv_sem,
            device_id=lax.bitwise_and(chip, 1) * half + lax.shift_right_logical(chip, 1),
            device_id_type=LOGICAL,
        ).start()
    mirror_copy = pltpu.make_async_remote_copy(
        merged.at[:, :, pl.ds(4, 4), :],
        mirror.at[:, :, pl.ds(4, 4), :],
        mirror_sem.at[0],
        mirror_sem.at[1],
        device_id=sibling,
        device_id_type=pl.DeviceIdType.MESH,
    )
    mirror_copy.start()

    tail = basis.at[pl.ds(1, VECTORS), 2, :, pl.ds(4, 4), :]
    tail_copy = pltpu.make_async_remote_copy(
        tail,
        tail,
        tail_sem.at[0],
        tail_sem.at[1],
        device_id=sibling,
        device_id_type=pl.DeviceIdType.MESH,
    )

    @pl.when(core == 1)
    def _():
        for n in range(2):
            for half in range(2):
                if n == 0:
                    arrived(halo_l.at[pl.ds(64 * half, 64), :], left_recv.at[n, half])
                else:
                    arrived(halo_lb.at[pl.ds(16 * half, 16), :], left_recv.at[n, half])
        for s in range(8):
            for i in range(2):
                value = halo_lb[pl.ds(16 * (s // 4) + 8 * i, 8), :]
                if s % 4:
                    value = pltpu.roll(value, 128 - DEPTH * (s % 4), 1)
                edge_b[pl.ds(16 * s + 8 * i, 8), :] = value

        def from_right(a, strided):
            if a == B:
                return edge_b[strided, :]
            g = PACKED.index(a)
            edge = halo_l[strided, :]
            return pltpu.roll(edge, 128 - DEPTH * g, 1) if g else edge

        fill(2, lane < DEPTH, from_right)
        build(2)
        for t in range(STEPS):
            load = lambda i: field[X0, 2, i]
            basis[0, 2, t] = jnp.zeros((8, 128), jnp.float32)
            basis[1, 2, t] = field[B, 2, t] - SCALE * operate(load, 2, t) - SHIFT * load(t)

        def grow_tail(k, carry):
            for t in range(STEPS):
                load = lambda i: basis[k + 1, 2, i]
                basis[k + 2, 2, t] = operate(load, 2, t) - basis[k, 2, t]
            return carry

        lax.fori_loop(0, RESTART, grow_tail, 0, unroll=3)
        tail_copy.start()

    mirror_copy.wait()

    @pl.when(core == 0)
    def _():
        tail_copy.wait_recv()

    upper = lane < 96
    near = row < 4
    is_first = (row * 0 + core) == 0
    in_first = near == is_first
    for k in range(VECTORS):
        for t in range(STEPS):
            own, other = merged[k, t], mirror[k, t]
            second = pltpu.roll(jnp.where(is_first, other, own), 4, 0)
            last = jnp.where(in_first, second, basis[k + 1, 2, t])
            joined[k, t] = jnp.where(upper, jnp.where(near, own, other), last)

    others = gathered.at[pl.ds(0, devices - 1)]
    everyone = pltpu.make_async_remote_copy(
        others, others, send_sem, recv_sem, device_id=sibling, device_id_type=pl.DeviceIdType.MESH
    )
    everyone.wait_recv()
    summed = jnp.sum(gathered[...], axis=0)
    summed = jnp.where(
        row < 4,
        jnp.broadcast_to(summed[0:1, :], (8, 128)),
        jnp.broadcast_to(summed[1:2, :], (8, 128)),
    )

    values = values_at_zero()
    columns = []
    for k in range(VECTORS):
        columns.append(
            [
                jnp.broadcast_to(
                    jnp.sum(
                        jnp.where(place_in == 2 * k + h, summed, 0.0), axis=1, keepdims=True
                    ),
                    (8, 128),
                )
                for h in range(2)
            ]
        )
    start = []
    for h in range(2):
        value = jnp.full((8, 128), values[8 * h], jnp.float32)
        for s in range(1, 8):
            value = jnp.where(row == s, values[8 * h + s], value)
        start.append(value)
    columns.append(list(start))

    def entry(column, i):
        return jnp.broadcast_to(column[i // 8][i % 8 : i % 8 + 1, :], (8, 128))

    for k in range(VECTORS):
        pivot = columns[k]
        inverse = 1.0 / entry(pivot, k)
        for j in range(k + 1, VECTORS + 1):
            factor = (entry(pivot, j) if j < VECTORS else entry(columns[j], k)) * inverse
            for h in range(2):
                columns[j][h] = columns[j][h] - pivot[h] * factor
            columns[j][k // 8] = jnp.where(row == k % 8, factor, columns[j][k // 8])
    u = columns[VECTORS]
    norm = jnp.sum(start[0] * u[0] + start[1] * u[1], axis=0, keepdims=True)
    inverse = jnp.broadcast_to(1.0 / norm, (8, 128))
    left_over = [entry(u, j) * inverse for j in range(VECTORS)]
    weights = [None] * RESTART
    for j in range(RESTART, 0, -1):
        value = left_over[j] * (-1.0 / SCALE)
        if j + 1 < RESTART:
            value = value - weights[j + 1]
        if j < RESTART:
            value = value - (SHIFT / SCALE) * weights[j]
        weights[j - 1] = value

    for t in range(STEPS):
        strided = pl.ds(t, 8, stride=STEPS)
        answer = jnp.where(
            near, block[X0, core, strided, :], pltpu.roll(block[X0, far, strided, :], 4, 0)
        )
        residual = jnp.zeros((8, 128), jnp.float32)
        for k in range(VECTORS):
            cells = joined[k, t]
            residual = residual + left_over[k] * cells
            if k < RESTART:
                answer = answer + weights[k] * cells
        out[0, strided, :] = answer
        out[1, strided, :] = residual

    everyone.wait_send()

    @pl.when(core == 1)
    def _():
        tail_copy.wait_send()

    for copy in sends:
        copy.wait_send()


def put_out(tiles, first, second, sem):
    core = lax.axis_index("gx")
    stores = []
    for o, output in enumerate((first, second)):
        for part in range(2):
            tile = core if part == 0 else 1 - core
            copy = pltpu.make_async_copy(
                tiles.at[o, pl.ds(64 * part, 64), :],
                output.at[:, pl.ds(pl.multiple_of(128 * tile, 128), 128)],
                sem.at[o, part],
            )
            copy.start()
            stores.append(copy)
    for copy in stores:
        copy.wait()


def per_device(sizes, *arrays):
    devices = 1
    for a in AXES:
        devices *= sizes[a]
    f32 = jnp.float32
    dma = pltpu.SemaphoreType.DMA
    shape = jax.ShapeDtypeStruct((64, 256), f32)
    tiles = pl.pallas_call(
        functools.partial(kernel, sizes),
        out_shape=pltpu.VMEM((2, 128, 128), f32),
        in_specs=[pl.BlockSpec(memory_space=pl.ANY)] * 5,
        out_specs=pl.BlockSpec(memory_space=pltpu.VMEM),
        scratch_shapes=[
            pltpu.VMEM((5, 2, 128, 128), f32),
            pltpu.VMEM((160, 128), f32),
            pltpu.VMEM((80, 128), f32),
            pltpu.VMEM((2, 128, 128), f32),
            pltpu.VMEM((64, 128), f32),
            pltpu.VMEM((128, 128), f32),
            pltpu.VMEM((32, 128), f32),
            pltpu.VMEM((128, 128), f32),
            pltpu.VMEM((9, 3, STEPS, 8, 128), f32),
            pltpu.VMEM((5, 3, STEPS, 8, 128), f32),
            pltpu.VMEM((VECTORS + 1, 3, STEPS, 8, 128), f32),
            pltpu.VMEM((VECTORS, STEPS, 8, 128), f32),
            pltpu.VMEM((VECTORS, STEPS, 8, 128), f32),
            pltpu.VMEM((VECTORS, STEPS, 8, 128), f32),
            pltpu.VMEM((VECTORS, VECTORS, 128), f32),
            pltpu.VMEM((devices, 2, 128), f32),
            pltpu.VMEM((2, 128), f32),
            dma((5, 2)),
            dma((2,)),
            dma((3,)),
            dma((3, 2)),
            dma((2,)),
            dma((2, 2)),
            dma((2,)),
            dma((2,)),
            dma,
            dma,
            pltpu.SemaphoreType.REGULAR((2,)),
        ],
        compiler_params=pltpu.CompilerParams(collective_id=0, has_side_effects=True),
    )(*arrays)
    return pl.pallas_call(
        put_out,
        out_shape=(shape, shape),
        in_specs=[pl.BlockSpec(memory_space=pltpu.VMEM)],
        out_specs=(pl.BlockSpec(memory_space=pl.ANY),) * 2,
        scratch_shapes=[dma((2, 2))],
    )(pltpu.with_memory_space_constraint(tiles, pltpu.VMEM))


def solution(mesh):
    counts = (4, 4, 4) if mesh.shape["gy"] == 64 else (1, 2, mesh.shape["gy"] // 2)
    torus = Mesh(mesh.devices.reshape((mesh.shape["gx"],) + counts), AXES)
    spec = P("gx", GY)
    return jax.shard_map(
        functools.partial(per_device, dict(torus.shape)),
        mesh=torus,
        in_specs=(spec,) * 5,
        out_specs=(spec, spec),
        check_vma=False,
    )
```

```python
import functools
import itertools

import jax
import jax.numpy as jnp
from jax import lax
from jax.experimental import pallas as pl
from jax.experimental.pallas import tpu as pltpu
from jax.sharding import Mesh
from jax.sharding import PartitionSpec as P

RESTART = 15
VECTORS = RESTART + 1
GY = ("gy_0", "gy_1", "gy_2")
AXES = ("gx",) + GY
LOGICAL = pl.DeviceIdType.LOGICAL
DEPTH = 32
GROUPS = 4
STEPS = 16
SHIFT, SCALE = 5.525, 2.65
B, X0, RE, VX, VY = 0, 1, 2, 3, 4
PACKED = (X0, RE, VX, VY)


def values_at_zero():
    values = [1.0, -SHIFT / SCALE]
    for _ in range(VECTORS - 2):
        values.append(-(SHIFT / SCALE) * values[-1] - values[-2])
    return values


def kernel(sizes, *refs):
    inputs = refs[:5]
    out = refs[5]
    (block, pack_r, pack_l, halo_r, halo_rb, halo_l, halo_lb, edge_b) = refs[6:14]
    (coef, field, basis, merged, mirror, joined, gram_parts, halves, gram_half) = refs[14:23]
    (gathered, share) = refs[23:25]
    (load_sem, swap_sem, right_send, right_recv, left_send, left_recv) = refs[25:31]
    (mirror_sem, tail_sem, send_sem, recv_sem, round_sem) = refs[31:]
    devices = 1
    for a in AXES:
        devices *= sizes[a]

    place = {a: lax.axis_index(a) for a in AXES}
    core = place["gx"]
    far = 1 - core
    sibling = {"gx": far}

    def along(step):
        total = sizes["gy_0"] * sizes["gy_1"] * sizes["gy_2"]
        flat = (place["gy_0"] * sizes["gy_1"] + place["gy_1"]) * sizes["gy_2"] + place["gy_2"]
        flat = lax.rem(flat + step + total, total)
        low = lax.rem(flat, sizes["gy_2"])
        rest = lax.div(flat, sizes["gy_2"])
        return lax.div(rest, sizes["gy_1"]), lax.rem(rest, sizes["gy_1"]), low

    right, left = along(1), along(-1)

    def at(chip, core_index):
        return {"gx": core_index, "gy_0": chip[0], "gy_1": chip[1], "gy_2": chip[2]}

    me = core
    for a in GY:
        me = me * sizes[a] + place[a]

    loads = []
    for a in range(5):
        for tile in range(2):
            loads.append(
                pltpu.make_async_copy(
                    inputs[a].at[:, pl.ds(128 * tile, 128)],
                    block.at[a, tile, pl.ds(0, 64), :],
                    load_sem.at[a, tile],
                )
            )
            loads[-1].start()
    barrier = pltpu.get_barrier_semaphore()
    peers = []
    for axes in (("gx", "gy_2"), ("gy_1",), ("gy_0",)):
        for offset in itertools.product(*[range(sizes[a]) for a in axes]):
            if any(offset):
                peers.append({a: lax.rem(place[a] + o, sizes[a]) for a, o in zip(axes, offset)})
    neighbours = [at(right, 0), at(right, 1), at(left, 0), at(left, 1)]

    def greet(devices_to, semaphore):
        for device in devices_to:
            pl.semaphore_signal(
                semaphore, inc=1, device_id=device, device_id_type=pl.DeviceIdType.MESH
            )

    greet(neighbours + peers, barrier)
    for load in loads:
        load.wait()

    lane = lax.broadcasted_iota(jnp.int32, (8, 128), 1)
    row = lax.broadcasted_iota(jnp.int32, (8, 128), 0)

    for n, (first, second) in enumerate(((X0, RE), (VX, VY), (B, B))):
        count = 64 if first != B else 32
        for i in range(count // 8):
            other = 8 * i if first != B else 32 + 8 * i
            pack_r[pl.ds(64 * n + 8 * i, 8), :] = jnp.where(
                lane >= 64,
                block[first, 1, pl.ds(8 * i, 8), :],
                pltpu.roll(block[second, 1, pl.ds(other, 8), :], 64, 1),
            )

    def pack_left(place_at, piece):
        value = piece(0)
        for g in range(1, GROUPS):
            inside = (lane >= DEPTH * g) & (lane < DEPTH * (g + 1))
            value = jnp.where(inside, pltpu.roll(piece(g), DEPTH * g, 1), value)
        pack_l[pl.ds(place_at, 8), :] = value

    for i in range(8):
        pack_left(8 * i, lambda g: block[PACKED[g], 0, pl.ds(8 * i, 8), :])
    for i in range(2):
        pack_left(64 + 8 * i, lambda g: block[B, 0, pl.ds(16 * g + 8 * i, 8), :])

    pl.semaphore_wait(barrier, len(neighbours) + len(peers))
    greet(peers, round_sem.at[0])

    sends = []
    for n in range(3):
        count = 64 if n < 2 else 32
        rows = pl.ds(pl.multiple_of(count * core, count), count)
        sends.append(
            pltpu.make_async_remote_copy(
                pack_r.at[pl.ds(64 * n, count), :],
                halo_r.at[n, rows, :] if n < 2 else halo_rb.at[rows, :],
                right_send.at[n],
                right_recv.at[n, core],
                device_id=at(right, 0),
                device_id_type=pl.DeviceIdType.MESH,
            )
        )
        sends[-1].start()
    swap = pltpu.make_async_remote_copy(
        block.at[:, :, pl.ds(0, 64), :],
        block.at[:, :, pl.ds(64, 64), :],
        swap_sem.at[0],
        swap_sem.at[1],
        device_id=sibling,
        device_id_type=pl.DeviceIdType.MESH,
    )
    swap.start()
    for n in range(2):
        count = 64 if n == 0 else 16
        rows = pl.ds(pl.multiple_of(count * far, count), count)
        sends.append(
            pltpu.make_async_remote_copy(
                pack_l.at[pl.ds(64 * n, count), :],
                halo_l.at[rows, :] if n == 0 else halo_lb.at[rows, :],
                left_send.at[n],
                left_recv.at[n, far],
                device_id=at(left, 1),
                device_id_type=pl.DeviceIdType.MESH,
            )
        )
        sends[-1].start()

    def arrived(landing, sem):
        pltpu.make_async_remote_copy(
            landing,
            landing,
            sem,
            sem,
            device_id=sibling,
            device_id_type=pl.DeviceIdType.MESH,
        ).wait_recv()

    inv = 1.0 / SCALE

    def row_shift(load, t):
        if t >= STEPS:
            return pltpu.roll(load(t - STEPS), 7, 0)
        if t < 0:
            return pltpu.roll(load(t + STEPS), 1, 0)
        return load(t)

    def column_shift(value, offset):
        return pltpu.roll(value, (-offset) % 128, 1)

    def fill(q, inside, edge):
        for a in range(5):
            for t in range(STEPS):
                strided = pl.ds(t, 8, stride=STEPS)
                value = block[a, core, strided, :]
                if inside is not None:
                    value = jnp.where(inside, edge(a, strided), value)
                field[a, q, t] = value

    def build(q):
        for t in range(STEPS):
            speed = lambda i: field[VX, q, i]
            here = speed(t)
            coef[0, q, t] = (field[RE, q, t] + (5.0 - SHIFT)) * inv
            coef[1, q, t] = (here + row_shift(speed, t + 1)) * (inv / 3.0) - 4.0 / 3.0 * inv
            coef[2, q, t] = (here + row_shift(speed, t - 1)) * (-inv / 3.0) - 4.0 / 3.0 * inv
            coef[3, q, t] = (here + row_shift(speed, t + 2)) * (-inv / 24.0) + inv / 12.0
            coef[4, q, t] = (here + row_shift(speed, t - 2)) * (inv / 24.0) + inv / 12.0
            here = field[VY, q, t]
            coef[5, q, t] = (here + column_shift(here, 1)) * (inv / 3.0) - 4.0 / 3.0 * inv
            coef[6, q, t] = (here + column_shift(here, -1)) * (-inv / 3.0) - 4.0 / 3.0 * inv
            coef[7, q, t] = (here + column_shift(here, 2)) * (-inv / 24.0) + inv / 12.0
            coef[8, q, t] = (here + column_shift(here, -2)) * (inv / 24.0) + inv / 12.0

    def operate(load, q, t):
        here = load(t)
        value = coef[0, q, t] * here
        value += coef[1, q, t] * row_shift(load, t + 1)
        value += coef[2, q, t] * row_shift(load, t - 1)
        value += coef[3, q, t] * row_shift(load, t + 2)
        value += coef[4, q, t] * row_shift(load, t - 2)
        value += coef[5, q, t] * column_shift(here, 1)
        value += coef[6, q, t] * column_shift(here, -1)
        value += coef[7, q, t] * column_shift(here, 2)
        value += coef[8, q, t] * column_shift(here, -2)
        return value

    middle = (lane >= 32) & (lane < 96)

    def keep(k, q, values):
        for t in range(STEPS):
            basis[k + 1, q, t] = values[t]
            if q == 0:
                merged[k, t] = jnp.where(middle, basis[k + 1, 1, t], values[t])
        for t in range(8):
            moved = pltpu.roll(values[t + 8], 64, 1)
            here = values[t]
            halves[q, k, t] = jnp.where(middle == (q == 1), here, moved)

    def steps(q):
        load = lambda i: field[X0, q, i]
        for t in range(STEPS):
            basis[0, q, t] = jnp.zeros((8, 128), jnp.float32)
        values = []
        for t in range(STEPS):
            values.append(field[B, q, t] - SCALE * operate(load, q, t) - SHIFT * load(t))
        keep(0, q, values)

        def grow(k, carry):
            load = lambda i: basis[k + 1, q, i]
            keep(k + 1, q, [operate(load, q, t) - basis[k, q, t] for t in range(STEPS)])
            return carry

        lax.fori_loop(0, RESTART, grow, 0, unroll=RESTART)

    def gram(q):
        size = 4
        for bi in range(VECTORS // size):
            for bj in range(bi + 1):
                pairs = [
                    (i, j)
                    for i in range(bi * size, bi * size + size)
                    for j in range(bj * size, bj * size + size)
                    if j <= i
                ]
                sums = {}
                for t in range(8):
                    need = sorted({i for pair in pairs for i in pair})
                    cells = {i: halves[q, i, t] for i in need}
                    for i, j in pairs:
                        product = cells[i] * cells[j]
                        sums[i, j] = product if t == 0 else sums[i, j] + product
                for i, j in pairs:
                    if q == 1:
                        gram_half[i * (i + 1) // 2 + j] = sums[i, j]
                        continue
                    total = sums[i, j] + gram_half[i * (i + 1) // 2 + j]
                    total = jnp.sum(total, axis=0, keepdims=True)
                    gram_parts[i, j : j + 1, :] = total
                    if i != j:
                        gram_parts[j, i : i + 1, :] = total

    swap.wait()
    fill(1, None, None)
    build(1)
    pl.semaphore_wait(round_sem.at[0], len(peers))
    greet(peers, round_sem.at[1])

    def steps_both():
        for t in range(STEPS):
            parts = []
            for q in range(2):
                load = lambda i: field[X0, q, i]
                basis[0, q, t] = jnp.zeros((8, 128), jnp.float32)
                parts.append(field[B, q, t] - SCALE * operate(load, q, t) - SHIFT * load(t))
                basis[1, q, t] = parts[q]
            merged[0, t] = jnp.where(middle, parts[1], parts[0])

        def grow(k, carry):
            for t in range(STEPS):
                parts = []
                for q in range(2):
                    load = lambda i: basis[k + 1, q, i]
                    parts.append(operate(load, q, t) - basis[k, q, t])
                    basis[k + 2, q, t] = parts[q]
                merged[k + 1, t] = jnp.where(middle, parts[1], parts[0])
            return carry

        lax.fori_loop(0, RESTART, grow, 0, unroll=RESTART)

    def gram_both():
        size = 4
        for bi in range(VECTORS // size):
            for bj in range(bi + 1):
                pairs = [
                    (i, j)
                    for i in range(bi * size, bi * size + size)
                    for j in range(bj * size, bj * size + size)
                    if j <= i
                ]
                sums = {}
                for t in range(STEPS):
                    need = sorted({i for pair in pairs for i in pair})
                    cells = {i: merged[i, t] for i in need}
                    for i, j in pairs:
                        product = cells[i] * cells[j]
                        sums[i, j] = product if t == 0 else sums[i, j] + product
                for i, j in pairs:
                    total = jnp.sum(sums[i, j], axis=0, keepdims=True)
                    gram_parts[i, j : j + 1, :] = total
                    if i != j:
                        gram_parts[j, i : i + 1, :] = total

    @pl.when(core == 1)
    def _():
        fill(0, lane >= 64, lambda a, strided: block[a, 0, strided, :])
        build(0)
        steps_both()
        gram_both()

    @pl.when(core == 0)
    def _():
        steps(1)
        gram(1)
        for n in range(3):
            for half in range(2):
                if n < 2:
                    arrived(halo_r.at[n, pl.ds(64 * half, 64), :], right_recv.at[n, half])
                else:
                    arrived(halo_rb.at[pl.ds(32 * half, 32), :], right_recv.at[n, half])
        for s in range(8):
            for i in range(2):
                value = halo_rb[pl.ds(32 * (s // 4) + 16 * (s % 2) + 8 * i, 8), :]
                if s % 4 >= 2:
                    value = pltpu.roll(value, 64, 1)
                edge_b[pl.ds(16 * s + 8 * i, 8), :] = value

        def from_left(a, strided):
            if a == B:
                return edge_b[strided, :]
            edge = halo_r[0 if a in (X0, RE) else 1, strided, :]
            return edge if a in (X0, VX) else pltpu.roll(edge, 64, 1)

        fill(0, lane >= 64, from_left)
        build(0)
        steps(0)
        gram(0)

    place_in = lane - 32 * (row & 3)
    packed = jnp.zeros((8, 128), jnp.float32)
    for k in range(VECTORS):
        for half in range(2):
            total = jnp.sum(gram_parts[k, 8 * half : 8 * half + 8, :], axis=1, keepdims=True)
            packed = jnp.where(place_in == 2 * k + half, total, packed)
    for r in range(2):
        line = jnp.sum(packed[4 * r : 4 * r + 4, :], axis=0, keepdims=True)
        share[r : r + 1, :] = line
        gathered[me, r : r + 1, :] = line

    pl.semaphore_wait(round_sem.at[1], len(peers))

    for o in range(1, devices):
        pltpu.make_async_remote_copy(
            share,
            gathered.at[me],
            send_sem,
            recv_sem,
            device_id=lax.bitwise_and(me + o, devices - 1),
            device_id_type=LOGICAL,
        ).start()
    mirror_copy = pltpu.make_async_remote_copy(
        merged.at[:, :, pl.ds(4, 4), :],
        mirror.at[:, :, pl.ds(4, 4), :],
        mirror_sem.at[0],
        mirror_sem.at[1],
        device_id=sibling,
        device_id_type=pl.DeviceIdType.MESH,
    )
    mirror_copy.start()

    tail = basis.at[pl.ds(1, VECTORS), 2, :, pl.ds(4, 4), :]
    tail_copy = pltpu.make_async_remote_copy(
        tail,
        tail,
        tail_sem.at[0],
        tail_sem.at[1],
        device_id=sibling,
        device_id_type=pl.DeviceIdType.MESH,
    )

    @pl.when(core == 1)
    def _():
        for n in range(2):
            for half in range(2):
                if n == 0:
                    arrived(halo_l.at[pl.ds(64 * half, 64), :], left_recv.at[n, half])
                else:
                    arrived(halo_lb.at[pl.ds(16 * half, 16), :], left_recv.at[n, half])
        for s in range(8):
            for i in range(2):
                value = halo_lb[pl.ds(16 * (s // 4) + 8 * i, 8), :]
                if s % 4:
                    value = pltpu.roll(value, 128 - DEPTH * (s % 4), 1)
                edge_b[pl.ds(16 * s + 8 * i, 8), :] = value

        def from_right(a, strided):
            if a == B:
                return edge_b[strided, :]
            g = PACKED.index(a)
            edge = halo_l[strided, :]
            return pltpu.roll(edge, 128 - DEPTH * g, 1) if g else edge

        fill(2, lane < DEPTH, from_right)
        build(2)
        for t in range(STEPS):
            load = lambda i: field[X0, 2, i]
            basis[0, 2, t] = jnp.zeros((8, 128), jnp.float32)
            basis[1, 2, t] = field[B, 2, t] - SCALE * operate(load, 2, t) - SHIFT * load(t)

        def grow_tail(k, carry):
            for t in range(STEPS):
                load = lambda i: basis[k + 1, 2, i]
                basis[k + 2, 2, t] = operate(load, 2, t) - basis[k, 2, t]
            return carry

        lax.fori_loop(0, RESTART, grow_tail, 0, unroll=3)
        tail_copy.start()

    mirror_copy.wait()

    @pl.when(core == 0)
    def _():
        tail_copy.wait_recv()

    upper = lane < 96
    near = row < 4
    is_first = (row * 0 + core) == 0
    in_first = near == is_first
    for k in range(VECTORS):
        for t in range(STEPS):
            own, other = merged[k, t], mirror[k, t]
            second = pltpu.roll(jnp.where(is_first, other, own), 4, 0)
            last = jnp.where(in_first, second, basis[k + 1, 2, t])
            joined[k, t] = jnp.where(upper, jnp.where(near, own, other), last)

    others = gathered.at[pl.ds(0, devices - 1)]
    everyone = pltpu.make_async_remote_copy(
        others, others, send_sem, recv_sem, device_id=sibling, device_id_type=pl.DeviceIdType.MESH
    )
    everyone.wait_recv()
    summed = jnp.sum(gathered[...], axis=0)
    summed = jnp.where(
        row < 4,
        jnp.broadcast_to(summed[0:1, :], (8, 128)),
        jnp.broadcast_to(summed[1:2, :], (8, 128)),
    )

    values = values_at_zero()
    columns = []
    for k in range(VECTORS):
        columns.append(
            [
                jnp.broadcast_to(
                    jnp.sum(
                        jnp.where(place_in == 2 * k + h, summed, 0.0), axis=1, keepdims=True
                    ),
                    (8, 128),
                )
                for h in range(2)
            ]
        )
    start = []
    for h in range(2):
        value = jnp.full((8, 128), values[8 * h], jnp.float32)
        for s in range(1, 8):
            value = jnp.where(row == s, values[8 * h + s], value)
        start.append(value)
    columns.append(list(start))

    def entry(column, i):
        return jnp.broadcast_to(column[i // 8][i % 8 : i % 8 + 1, :], (8, 128))

    for k in range(VECTORS):
        pivot = columns[k]
        inverse = 1.0 / entry(pivot, k)
        for j in range(k + 1, VECTORS + 1):
            factor = (entry(pivot, j) if j < VECTORS else entry(columns[j], k)) * inverse
            for h in range(2):
                columns[j][h] = columns[j][h] - pivot[h] * factor
            columns[j][k // 8] = jnp.where(row == k % 8, factor, columns[j][k // 8])
    u = columns[VECTORS]
    norm = jnp.sum(start[0] * u[0] + start[1] * u[1], axis=0, keepdims=True)
    inverse = jnp.broadcast_to(1.0 / norm, (8, 128))
    left_over = [entry(u, j) * inverse for j in range(VECTORS)]
    weights = [None] * RESTART
    for j in range(RESTART, 0, -1):
        value = left_over[j] * (-1.0 / SCALE)
        if j + 1 < RESTART:
            value = value - weights[j + 1]
        if j < RESTART:
            value = value - (SHIFT / SCALE) * weights[j]
        weights[j - 1] = value

    for t in range(STEPS):
        strided = pl.ds(t, 8, stride=STEPS)
        answer = jnp.where(
            near, block[X0, core, strided, :], pltpu.roll(block[X0, far, strided, :], 4, 0)
        )
        residual = jnp.zeros((8, 128), jnp.float32)
        for k in range(VECTORS):
            cells = joined[k, t]
            residual = residual + left_over[k] * cells
            if k < RESTART:
                answer = answer + weights[k] * cells
        out[0, strided, :] = answer
        out[1, strided, :] = residual

    everyone.wait_send()

    @pl.when(core == 1)
    def _():
        tail_copy.wait_send()

    for copy in sends:
        copy.wait_send()


def put_out(tiles, first, second, sem):
    core = lax.axis_index("gx")
    stores = []
    for o, output in enumerate((first, second)):
        for part in range(2):
            tile = core if part == 0 else 1 - core
            copy = pltpu.make_async_copy(
                tiles.at[o, pl.ds(64 * part, 64), :],
                output.at[:, pl.ds(pl.multiple_of(128 * tile, 128), 128)],
                sem.at[o, part],
            )
            copy.start()
            stores.append(copy)
    for copy in stores:
        copy.wait()


def per_device(sizes, *arrays):
    devices = 1
    for a in AXES:
        devices *= sizes[a]
    f32 = jnp.float32
    dma = pltpu.SemaphoreType.DMA
    shape = jax.ShapeDtypeStruct((64, 256), f32)
    tiles = pl.pallas_call(
        functools.partial(kernel, sizes),
        out_shape=pltpu.VMEM((2, 128, 128), f32),
        in_specs=[pl.BlockSpec(memory_space=pl.ANY)] * 5,
        out_specs=pl.BlockSpec(memory_space=pltpu.VMEM),
        scratch_shapes=[
            pltpu.VMEM((5, 2, 128, 128), f32),
            pltpu.VMEM((160, 128), f32),
            pltpu.VMEM((80, 128), f32),
            pltpu.VMEM((2, 128, 128), f32),
            pltpu.VMEM((64, 128), f32),
            pltpu.VMEM((128, 128), f32),
            pltpu.VMEM((32, 128), f32),
            pltpu.VMEM((128, 128), f32),
            pltpu.VMEM((9, 3, STEPS, 8, 128), f32),
            pltpu.VMEM((5, 3, STEPS, 8, 128), f32),
            pltpu.VMEM((VECTORS + 1, 3, STEPS, 8, 128), f32),
            pltpu.VMEM((VECTORS, STEPS, 8, 128), f32),
            pltpu.VMEM((VECTORS, STEPS, 8, 128), f32),
            pltpu.VMEM((VECTORS, STEPS, 8, 128), f32),
            pltpu.VMEM((VECTORS, VECTORS, 128), f32),
            pltpu.VMEM((2, VECTORS, 8, 8, 128), f32),
            pltpu.VMEM((VECTORS * (VECTORS + 1) // 2, 8, 128), f32),
            pltpu.VMEM((devices, 2, 128), f32),
            pltpu.VMEM((2, 128), f32),
            dma((5, 2)),
            dma((2,)),
            dma((3,)),
            dma((3, 2)),
            dma((2,)),
            dma((2, 2)),
            dma((2,)),
            dma((2,)),
            dma,
            dma,
            pltpu.SemaphoreType.REGULAR((2,)),
        ],
        compiler_params=pltpu.CompilerParams(collective_id=0, has_side_effects=True),
    )(*arrays)
    return pl.pallas_call(
        put_out,
        out_shape=(shape, shape),
        in_specs=[pl.BlockSpec(memory_space=pltpu.VMEM)],
        out_specs=(pl.BlockSpec(memory_space=pl.ANY),) * 2,
        scratch_shapes=[dma((2, 2))],
    )(pltpu.with_memory_space_constraint(tiles, pltpu.VMEM))


def solution(mesh):
    counts = (4, 4, 4) if mesh.shape["gy"] == 64 else (1, 2, mesh.shape["gy"] // 2)
    torus = Mesh(mesh.devices.reshape((mesh.shape["gx"],) + counts), AXES)
    spec = P("gx", GY)
    return jax.shard_map(
        functools.partial(per_device, dict(torus.shape)),
        mesh=torus,
        in_specs=(spec,) * 5,
        out_specs=(spec, spec),
        check_vma=False,
    )
```

```python
import functools
import itertools

import jax
import jax.numpy as jnp
from jax import lax
from jax.experimental import pallas as pl
from jax.experimental.pallas import tpu as pltpu
from jax.sharding import Mesh
from jax.sharding import PartitionSpec as P

RESTART = 15
VECTORS = RESTART + 1
GY = ("gy_0", "gy_1", "gy_2")
AXES = ("gx",) + GY
LOGICAL = pl.DeviceIdType.LOGICAL
DEPTH = 32
GROUPS = 4
STEPS = 16
SHIFT, SCALE = 5.525, 2.65
B, X0, RE, VX, VY = 0, 1, 2, 3, 4
PACKED = (X0, RE, VX, VY)


def values_at_zero():
    values = [1.0, -SHIFT / SCALE]
    for _ in range(VECTORS - 2):
        values.append(-(SHIFT / SCALE) * values[-1] - values[-2])
    return values


def kernel(sizes, *refs):
    inputs = refs[:5]
    out = refs[5]
    (block, pack_r, pack_l, halo_r, halo_rb, halo_l, halo_lb, edge_b) = refs[6:14]
    (coef, field, basis, merged, mirror, joined, gram_parts, halves, gram_half) = refs[14:23]
    (gathered, share) = refs[23:25]
    (load_sem, swap_sem, right_send, right_recv, left_send, left_recv) = refs[25:31]
    (mirror_sem, tail_sem, send_sem, recv_sem, round_sem) = refs[31:]
    devices = 1
    for a in AXES:
        devices *= sizes[a]

    place = {a: lax.axis_index(a) for a in AXES}
    core = place["gx"]
    far = 1 - core
    sibling = {"gx": far}

    def along(step):
        total = sizes["gy_0"] * sizes["gy_1"] * sizes["gy_2"]
        flat = (place["gy_0"] * sizes["gy_1"] + place["gy_1"]) * sizes["gy_2"] + place["gy_2"]
        flat = lax.rem(flat + step + total, total)
        low = lax.rem(flat, sizes["gy_2"])
        rest = lax.div(flat, sizes["gy_2"])
        return lax.div(rest, sizes["gy_1"]), lax.rem(rest, sizes["gy_1"]), low

    right, left = along(1), along(-1)

    def at(chip, core_index):
        return {"gx": core_index, "gy_0": chip[0], "gy_1": chip[1], "gy_2": chip[2]}

    me = core
    for a in GY:
        me = me * sizes[a] + place[a]

    loads = []
    for a in range(5):
        for tile in range(2):
            loads.append(
                pltpu.make_async_copy(
                    inputs[a].at[:, pl.ds(128 * tile, 128)],
                    block.at[a, tile, pl.ds(0, 64), :],
                    load_sem.at[a, tile],
                )
            )
            loads[-1].start()
    barrier = pltpu.get_barrier_semaphore()
    peers = []
    for axes in (("gx", "gy_2"), ("gy_1",), ("gy_0",)):
        for offset in itertools.product(*[range(sizes[a]) for a in axes]):
            if any(offset):
                peers.append({a: lax.rem(place[a] + o, sizes[a]) for a, o in zip(axes, offset)})
    neighbours = [at(right, 0), at(right, 1), at(left, 0), at(left, 1)]

    def greet(devices_to, semaphore):
        for device in devices_to:
            pl.semaphore_signal(
                semaphore, inc=1, device_id=device, device_id_type=pl.DeviceIdType.MESH
            )

    greet(neighbours + peers, barrier)
    for load in loads:
        load.wait()

    lane = lax.broadcasted_iota(jnp.int32, (8, 128), 1)
    row = lax.broadcasted_iota(jnp.int32, (8, 128), 0)

    for n, (first, second) in enumerate(((X0, RE), (VX, VY), (B, B))):
        count = 64 if first != B else 32
        for i in range(count // 8):
            other = 8 * i if first != B else 32 + 8 * i
            pack_r[pl.ds(64 * n + 8 * i, 8), :] = jnp.where(
                lane >= 64,
                block[first, 1, pl.ds(8 * i, 8), :],
                pltpu.roll(block[second, 1, pl.ds(other, 8), :], 64, 1),
            )

    def pack_left(place_at, piece):
        value = piece(0)
        for g in range(1, GROUPS):
            inside = (lane >= DEPTH * g) & (lane < DEPTH * (g + 1))
            value = jnp.where(inside, pltpu.roll(piece(g), DEPTH * g, 1), value)
        pack_l[pl.ds(place_at, 8), :] = value

    for i in range(8):
        pack_left(8 * i, lambda g: block[PACKED[g], 0, pl.ds(8 * i, 8), :])
    for i in range(2):
        pack_left(64 + 8 * i, lambda g: block[B, 0, pl.ds(16 * g + 8 * i, 8), :])

    pl.semaphore_wait(barrier, len(neighbours) + len(peers))
    greet(peers, round_sem.at[0])

    sends = []
    for n in range(3):
        count = 64 if n < 2 else 32
        rows = pl.ds(pl.multiple_of(count * core, count), count)
        sends.append(
            pltpu.make_async_remote_copy(
                pack_r.at[pl.ds(64 * n, count), :],
                halo_r.at[n, rows, :] if n < 2 else halo_rb.at[rows, :],
                right_send.at[n],
                right_recv.at[n, core],
                device_id=at(right, 0),
                device_id_type=pl.DeviceIdType.MESH,
            )
        )
        sends[-1].start()
    swap = pltpu.make_async_remote_copy(
        block.at[:, :, pl.ds(0, 64), :],
        block.at[:, :, pl.ds(64, 64), :],
        swap_sem.at[0],
        swap_sem.at[1],
        device_id=sibling,
        device_id_type=pl.DeviceIdType.MESH,
    )
    swap.start()
    for n in range(2):
        count = 64 if n == 0 else 16
        rows = pl.ds(pl.multiple_of(count * far, count), count)
        sends.append(
            pltpu.make_async_remote_copy(
                pack_l.at[pl.ds(64 * n, count), :],
                halo_l.at[rows, :] if n == 0 else halo_lb.at[rows, :],
                left_send.at[n],
                left_recv.at[n, far],
                device_id=at(left, 1),
                device_id_type=pl.DeviceIdType.MESH,
            )
        )
        sends[-1].start()

    def arrived(landing, sem):
        pltpu.make_async_remote_copy(
            landing,
            landing,
            sem,
            sem,
            device_id=sibling,
            device_id_type=pl.DeviceIdType.MESH,
        ).wait_recv()

    inv = 1.0 / SCALE

    def row_shift(load, t):
        if t >= STEPS:
            return pltpu.roll(load(t - STEPS), 7, 0)
        if t < 0:
            return pltpu.roll(load(t + STEPS), 1, 0)
        return load(t)

    def column_shift(value, offset):
        return pltpu.roll(value, (-offset) % 128, 1)

    def fill(q, inside, edge):
        for a in range(5):
            for t in range(STEPS):
                strided = pl.ds(t, 8, stride=STEPS)
                value = block[a, core, strided, :]
                if inside is not None:
                    value = jnp.where(inside, edge(a, strided), value)
                field[a, q, t] = value

    def build(q):
        for t in range(STEPS):
            speed = lambda i: field[VX, q, i]
            here = speed(t)
            coef[0, q, t] = (field[RE, q, t] + (5.0 - SHIFT)) * inv
            coef[1, q, t] = (here + row_shift(speed, t + 1)) * (inv / 3.0) - 4.0 / 3.0 * inv
            coef[2, q, t] = (here + row_shift(speed, t - 1)) * (-inv / 3.0) - 4.0 / 3.0 * inv
            coef[3, q, t] = (here + row_shift(speed, t + 2)) * (-inv / 24.0) + inv / 12.0
            coef[4, q, t] = (here + row_shift(speed, t - 2)) * (inv / 24.0) + inv / 12.0
            here = field[VY, q, t]
            coef[5, q, t] = (here + column_shift(here, 1)) * (inv / 3.0) - 4.0 / 3.0 * inv
            coef[6, q, t] = (here + column_shift(here, 1)) * (-inv / 3.0) - 4.0 / 3.0 * inv
            coef[7, q, t] = (here + column_shift(here, 2)) * (-inv / 24.0) + inv / 12.0
            coef[8, q, t] = (here + column_shift(here, 2)) * (inv / 24.0) + inv / 12.0

    def operate(load, q, t):
        here = load(t)
        value = coef[0, q, t] * here
        value += coef[1, q, t] * row_shift(load, t + 1)
        value += coef[2, q, t] * row_shift(load, t - 1)
        value += coef[3, q, t] * row_shift(load, t + 2)
        value += coef[4, q, t] * row_shift(load, t - 2)
        value += coef[5, q, t] * column_shift(here, 1)
        value += column_shift(coef[6, q, t] * here, -1)
        value += coef[7, q, t] * column_shift(here, 2)
        value += column_shift(coef[8, q, t] * here, -2)
        return value

    middle = (lane >= 32) & (lane < 96)

    def keep(k, q, values):
        for t in range(STEPS):
            basis[k + 1, q, t] = values[t]
            if q == 0:
                merged[k, t] = jnp.where(middle, basis[k + 1, 1, t], values[t])
        for t in range(8):
            moved = pltpu.roll(values[t + 8], 64, 1)
            here = values[t]
            halves[q, k, t] = jnp.where(middle == (q == 1), here, moved)

    def steps(q):
        load = lambda i: field[X0, q, i]
        for t in range(STEPS):
            basis[0, q, t] = jnp.zeros((8, 128), jnp.float32)
        values = []
        for t in range(STEPS):
            values.append(field[B, q, t] - SCALE * operate(load, q, t) - SHIFT * load(t))
        keep(0, q, values)

        def grow(k, carry):
            load = lambda i: basis[k + 1, q, i]
            keep(k + 1, q, [operate(load, q, t) - basis[k, q, t] for t in range(STEPS)])
            return carry

        lax.fori_loop(0, RESTART, grow, 0, unroll=RESTART)

    def gram(q):
        size = 4
        for bi in range(VECTORS // size):
            for bj in range(bi + 1):
                pairs = [
                    (i, j)
                    for i in range(bi * size, bi * size + size)
                    for j in range(bj * size, bj * size + size)
                    if j <= i
                ]
                sums = {}
                for t in range(8):
                    need = sorted({i for pair in pairs for i in pair})
                    cells = {i: halves[q, i, t] for i in need}
                    for i, j in pairs:
                        product = cells[i] * cells[j]
                        sums[i, j] = product if t == 0 else sums[i, j] + product
                for i, j in pairs:
                    if q == 1:
                        gram_half[i * (i + 1) // 2 + j] = sums[i, j]
                        continue
                    total = sums[i, j] + gram_half[i * (i + 1) // 2 + j]
                    total = jnp.sum(total, axis=0, keepdims=True)
                    gram_parts[i, j : j + 1, :] = total
                    if i != j:
                        gram_parts[j, i : i + 1, :] = total

    swap.wait()
    fill(1, None, None)
    build(1)
    pl.semaphore_wait(round_sem.at[0], len(peers))
    greet(peers, round_sem.at[1])

    def steps_both():
        for t in range(STEPS):
            parts = []
            for q in range(2):
                load = lambda i: field[X0, q, i]
                basis[0, q, t] = jnp.zeros((8, 128), jnp.float32)
                parts.append(field[B, q, t] - SCALE * operate(load, q, t) - SHIFT * load(t))
                basis[1, q, t] = parts[q]
            merged[0, t] = jnp.where(middle, parts[1], parts[0])

        def grow(k, carry):
            for t in range(STEPS):
                parts = []
                for q in range(2):
                    load = lambda i: basis[k + 1, q, i]
                    parts.append(operate(load, q, t) - basis[k, q, t])
                    basis[k + 2, q, t] = parts[q]
                merged[k + 1, t] = jnp.where(middle, parts[1], parts[0])
            return carry

        lax.fori_loop(0, RESTART, grow, 0, unroll=RESTART)

    def gram_both():
        size = 4
        for bi in range(VECTORS // size):
            for bj in range(bi + 1):
                pairs = [
                    (i, j)
                    for i in range(bi * size, bi * size + size)
                    for j in range(bj * size, bj * size + size)
                    if j <= i
                ]
                sums = {}
                for t in range(STEPS):
                    need = sorted({i for pair in pairs for i in pair})
                    cells = {i: merged[i, t] for i in need}
                    for i, j in pairs:
                        product = cells[i] * cells[j]
                        sums[i, j] = product if t == 0 else sums[i, j] + product
                for i, j in pairs:
                    total = jnp.sum(sums[i, j], axis=0, keepdims=True)
                    gram_parts[i, j : j + 1, :] = total
                    if i != j:
                        gram_parts[j, i : i + 1, :] = total

    @pl.when(core == 1)
    def _():
        fill(0, lane >= 64, lambda a, strided: block[a, 0, strided, :])
        build(0)
        steps_both()
        gram_both()

    @pl.when(core == 0)
    def _():
        steps(1)
        gram(1)
        for n in range(3):
            for half in range(2):
                if n < 2:
                    arrived(halo_r.at[n, pl.ds(64 * half, 64), :], right_recv.at[n, half])
                else:
                    arrived(halo_rb.at[pl.ds(32 * half, 32), :], right_recv.at[n, half])
        for s in range(8):
            for i in range(2):
                value = halo_rb[pl.ds(32 * (s // 4) + 16 * (s % 2) + 8 * i, 8), :]
                if s % 4 >= 2:
                    value = pltpu.roll(value, 64, 1)
                edge_b[pl.ds(16 * s + 8 * i, 8), :] = value

        def from_left(a, strided):
            if a == B:
                return edge_b[strided, :]
            edge = halo_r[0 if a in (X0, RE) else 1, strided, :]
            return edge if a in (X0, VX) else pltpu.roll(edge, 64, 1)

        fill(0, lane >= 64, from_left)
        build(0)
        steps(0)
        gram(0)

    place_in = lane - 32 * (row & 3)
    packed = jnp.zeros((8, 128), jnp.float32)
    for k in range(VECTORS):
        for half in range(2):
            total = jnp.sum(gram_parts[k, 8 * half : 8 * half + 8, :], axis=1, keepdims=True)
            packed = jnp.where(place_in == 2 * k + half, total, packed)
    for r in range(2):
        line = jnp.sum(packed[4 * r : 4 * r + 4, :], axis=0, keepdims=True)
        share[r : r + 1, :] = line
        gathered[me, r : r + 1, :] = line

    pl.semaphore_wait(round_sem.at[1], len(peers))

    for o in range(1, devices):
        pltpu.make_async_remote_copy(
            share,
            gathered.at[me],
            send_sem,
            recv_sem,
            device_id=lax.bitwise_and(me + o, devices - 1),
            device_id_type=LOGICAL,
        ).start()
    mirror_copy = pltpu.make_async_remote_copy(
        merged.at[:, :, pl.ds(4, 4), :],
        mirror.at[:, :, pl.ds(4, 4), :],
        mirror_sem.at[0],
        mirror_sem.at[1],
        device_id=sibling,
        device_id_type=pl.DeviceIdType.MESH,
    )
    mirror_copy.start()

    tail = basis.at[pl.ds(1, VECTORS), 2, :, pl.ds(4, 4), :]
    tail_copy = pltpu.make_async_remote_copy(
        tail,
        tail,
        tail_sem.at[0],
        tail_sem.at[1],
        device_id=sibling,
        device_id_type=pl.DeviceIdType.MESH,
    )

    @pl.when(core == 1)
    def _():
        for n in range(2):
            for half in range(2):
                if n == 0:
                    arrived(halo_l.at[pl.ds(64 * half, 64), :], left_recv.at[n, half])
                else:
                    arrived(halo_lb.at[pl.ds(16 * half, 16), :], left_recv.at[n, half])
        for s in range(8):
            for i in range(2):
                value = halo_lb[pl.ds(16 * (s // 4) + 8 * i, 8), :]
                if s % 4:
                    value = pltpu.roll(value, 128 - DEPTH * (s % 4), 1)
                edge_b[pl.ds(16 * s + 8 * i, 8), :] = value

        def from_right(a, strided):
            if a == B:
                return edge_b[strided, :]
            g = PACKED.index(a)
            edge = halo_l[strided, :]
            return pltpu.roll(edge, 128 - DEPTH * g, 1) if g else edge

        fill(2, lane < DEPTH, from_right)
        build(2)
        for t in range(STEPS):
            load = lambda i: field[X0, 2, i]
            basis[0, 2, t] = jnp.zeros((8, 128), jnp.float32)
            basis[1, 2, t] = field[B, 2, t] - SCALE * operate(load, 2, t) - SHIFT * load(t)

        def grow_tail(k, carry):
            for t in range(STEPS):
                load = lambda i: basis[k + 1, 2, i]
                basis[k + 2, 2, t] = operate(load, 2, t) - basis[k, 2, t]
            return carry

        lax.fori_loop(0, RESTART, grow_tail, 0, unroll=3)
        tail_copy.start()

    mirror_copy.wait()

    @pl.when(core == 0)
    def _():
        tail_copy.wait_recv()

    upper = lane < 96
    near = row < 4
    is_first = (row * 0 + core) == 0
    in_first = near == is_first
    for k in range(VECTORS):
        for t in range(STEPS):
            own, other = merged[k, t], mirror[k, t]
            second = pltpu.roll(jnp.where(is_first, other, own), 4, 0)
            last = jnp.where(in_first, second, basis[k + 1, 2, t])
            joined[k, t] = jnp.where(upper, jnp.where(near, own, other), last)

    others = gathered.at[pl.ds(0, devices - 1)]
    everyone = pltpu.make_async_remote_copy(
        others, others, send_sem, recv_sem, device_id=sibling, device_id_type=pl.DeviceIdType.MESH
    )
    everyone.wait_recv()
    summed = jnp.sum(gathered[...], axis=0)
    summed = jnp.where(
        row < 4,
        jnp.broadcast_to(summed[0:1, :], (8, 128)),
        jnp.broadcast_to(summed[1:2, :], (8, 128)),
    )

    values = values_at_zero()
    columns = []
    for k in range(VECTORS):
        columns.append(
            [
                jnp.broadcast_to(
                    jnp.sum(
                        jnp.where(place_in == 2 * k + h, summed, 0.0), axis=1, keepdims=True
                    ),
                    (8, 128),
                )
                for h in range(2)
            ]
        )
    start = []
    for h in range(2):
        value = jnp.full((8, 128), values[8 * h], jnp.float32)
        for s in range(1, 8):
            value = jnp.where(row == s, values[8 * h + s], value)
        start.append(value)
    columns.append(list(start))

    def entry(column, i):
        return jnp.broadcast_to(column[i // 8][i % 8 : i % 8 + 1, :], (8, 128))

    for k in range(VECTORS):
        pivot = columns[k]
        inverse = 1.0 / entry(pivot, k)
        for j in range(k + 1, VECTORS + 1):
            factor = (entry(pivot, j) if j < VECTORS else entry(columns[j], k)) * inverse
            for h in range(2):
                columns[j][h] = columns[j][h] - pivot[h] * factor
            columns[j][k // 8] = jnp.where(row == k % 8, factor, columns[j][k // 8])
    u = columns[VECTORS]
    norm = jnp.sum(start[0] * u[0] + start[1] * u[1], axis=0, keepdims=True)
    inverse = jnp.broadcast_to(1.0 / norm, (8, 128))
    left_over = [entry(u, j) * inverse for j in range(VECTORS)]
    weights = [None] * RESTART
    for j in range(RESTART, 0, -1):
        value = left_over[j] * (-1.0 / SCALE)
        if j + 1 < RESTART:
            value = value - weights[j + 1]
        if j < RESTART:
            value = value - (SHIFT / SCALE) * weights[j]
        weights[j - 1] = value

    for t in range(STEPS):
        strided = pl.ds(t, 8, stride=STEPS)
        answer = jnp.where(
            near, block[X0, core, strided, :], pltpu.roll(block[X0, far, strided, :], 4, 0)
        )
        residual = jnp.zeros((8, 128), jnp.float32)
        for k in range(VECTORS):
            cells = joined[k, t]
            residual = residual + left_over[k] * cells
            if k < RESTART:
                answer = answer + weights[k] * cells
        out[0, strided, :] = answer
        out[1, strided, :] = residual

    everyone.wait_send()

    @pl.when(core == 1)
    def _():
        tail_copy.wait_send()

    for copy in sends:
        copy.wait_send()


def put_out(tiles, first, second, sem):
    core = lax.axis_index("gx")
    stores = []
    for o, output in enumerate((first, second)):
        for part in range(2):
            tile = core if part == 0 else 1 - core
            copy = pltpu.make_async_copy(
                tiles.at[o, pl.ds(64 * part, 64), :],
                output.at[:, pl.ds(pl.multiple_of(128 * tile, 128), 128)],
                sem.at[o, part],
            )
            copy.start()
            stores.append(copy)
    for copy in stores:
        copy.wait()


def per_device(sizes, *arrays):
    devices = 1
    for a in AXES:
        devices *= sizes[a]
    f32 = jnp.float32
    dma = pltpu.SemaphoreType.DMA
    shape = jax.ShapeDtypeStruct((64, 256), f32)
    tiles = pl.pallas_call(
        functools.partial(kernel, sizes),
        out_shape=pltpu.VMEM((2, 128, 128), f32),
        in_specs=[pl.BlockSpec(memory_space=pl.ANY)] * 5,
        out_specs=pl.BlockSpec(memory_space=pltpu.VMEM),
        scratch_shapes=[
            pltpu.VMEM((5, 2, 128, 128), f32),
            pltpu.VMEM((160, 128), f32),
            pltpu.VMEM((80, 128), f32),
            pltpu.VMEM((2, 128, 128), f32),
            pltpu.VMEM((64, 128), f32),
            pltpu.VMEM((128, 128), f32),
            pltpu.VMEM((32, 128), f32),
            pltpu.VMEM((128, 128), f32),
            pltpu.VMEM((9, 3, STEPS, 8, 128), f32),
            pltpu.VMEM((5, 3, STEPS, 8, 128), f32),
            pltpu.VMEM((VECTORS + 1, 3, STEPS, 8, 128), f32),
            pltpu.VMEM((VECTORS, STEPS, 8, 128), f32),
            pltpu.VMEM((VECTORS, STEPS, 8, 128), f32),
            pltpu.VMEM((VECTORS, STEPS, 8, 128), f32),
            pltpu.VMEM((VECTORS, VECTORS, 128), f32),
            pltpu.VMEM((2, VECTORS, 8, 8, 128), f32),
            pltpu.VMEM((VECTORS * (VECTORS + 1) // 2, 8, 128), f32),
            pltpu.VMEM((devices, 2, 128), f32),
            pltpu.VMEM((2, 128), f32),
            dma((5, 2)),
            dma((2,)),
            dma((3,)),
            dma((3, 2)),
            dma((2,)),
            dma((2, 2)),
            dma((2,)),
            dma((2,)),
            dma,
            dma,
            pltpu.SemaphoreType.REGULAR((2,)),
        ],
        compiler_params=pltpu.CompilerParams(collective_id=0, has_side_effects=True),
    )(*arrays)
    return pl.pallas_call(
        put_out,
        out_shape=(shape, shape),
        in_specs=[pl.BlockSpec(memory_space=pltpu.VMEM)],
        out_specs=(pl.BlockSpec(memory_space=pl.ANY),) * 2,
        scratch_shapes=[dma((2, 2))],
    )(pltpu.with_memory_space_constraint(tiles, pltpu.VMEM))


def solution(mesh):
    counts = (4, 4, 4) if mesh.shape["gy"] == 64 else (1, 2, mesh.shape["gy"] // 2)
    torus = Mesh(mesh.devices.reshape((mesh.shape["gx"],) + counts), AXES)
    spec = P("gx", GY)
    return jax.shard_map(
        functools.partial(per_device, dict(torus.shape)),
        mesh=torus,
        in_specs=(spec,) * 5,
        out_specs=(spec, spec),
        check_vma=False,
    )
```
